32 devices in a mesh: rep: 8 (over y, x, core), tp: 4 (over z).
Axes of the slice: x: 2, y: 2, z: 4, core: 2. Of those that a mesh axis runs over, the one named last changes fastest.
Arguments:
- queries: bfloat16 [2048, 4096], P('rep', 'tp'), may hold values from -120 to 120
- keys_new: bfloat16 [2048, 1024], P('rep', 'tp'), may hold values from -7 to 7
- values_new: bfloat16 [2048, 1024], P('rep', 'tp'), may hold values from -6 to 6
- caches: bfloat16 [16, 2, 4096, 1024], P('rep', None, None, 'tp'), may hold values from -6 to 6
- lengths: int32 [8, 2], replicated, may hold values from 128 to 4096, as said below
- moving: int32 [8], replicated, may hold values from 0 to 1
- destination: int32 [8], replicated, may hold values from 0 to 7, each once
- out_weight: bfloat16 [4096, 4096], P('tp'), may hold values from -0.09375 to 0.09375
Outputs:
- mixed: bfloat16 [2048, 4096], P('rep', 'tp')
- held_cache: bfloat16 [16, 2, 4096, 1024], P('rep', None, None, 'tp')
The draws below stay inside these ranges and needn't reach their ends.
Inputs may be any that keep to these rules, and one draw needn't show every extreme that they name: `lengths`: multiples of 128; in every draw some slot holds 4096 and some 128. `destination`: each replica receives exactly one failing candidate; it takes the slot that its own failing candidate leaves.
All inputs are finite; a program needn't handle non-finite values.
Results may differ from the reference program's by a relative error of at most 0.014.
Values may be sent and summed in bfloat16 or wider, within the bound.
A program may use at most 64 MiB of HBM per device.

```python
import jax
import jax.numpy as jnp
from jax import lax

HEADS = 32
KV_HEADS = 8
HEAD = 128
OUT = 4096
SPAN = 128
SLOTS = 2
CACHE = 4096
ROWS = 2048
N_REP = 8


def fresh_keys(key):
    base = jax.random.normal(jax.random.fold_in(key, 7), (ROWS, KV_HEADS, HEAD), jnp.float32)
    return jnp.clip(base, -6.0, 6.0)


def draw_keys_new(key, part):
    base = fresh_keys(key)
    return base.reshape(ROWS, KV_HEADS * HEAD).astype(jnp.bfloat16)


def draw_queries(key, part):
    base = jnp.clip(jax.random.normal(jax.random.fold_in(key, 11), (ROWS, HEADS, HEAD), jnp.float32), -6.0, 6.0)
    return base.reshape(ROWS, HEADS * HEAD).astype(jnp.bfloat16)


def draw_lengths(key, part):
    blocks = jax.random.randint(jax.random.fold_in(key, 3), (N_REP * SLOTS,), 1, CACHE // 128 + 1)
    picked = jax.random.permutation(jax.random.fold_in(key, 5), N_REP * SLOTS)
    blocks = blocks.at[picked[0]].set(CACHE // 128)
    blocks = blocks.at[picked[1]].set(1)
    return (blocks * 128).reshape(N_REP, SLOTS).astype(jnp.int32)


def with_ends(values, stream_key, smallest, high):
    spot = [jax.random.randint(jax.random.fold_in(stream_key, axis), (), 0, length) for axis, length in enumerate(values.shape)]
    longest = values.shape.index(max(values.shape))
    beside = spot[:longest] + [(spot[longest] + 1) % values.shape[longest]] + spot[longest + 1:]
    return values.at[tuple(spot)].set(smallest).at[tuple(beside)].set(high)


def level_of(own_key, extent, pieces, least, top_value):
    def one(dim, shards_of):
        heights = jax.random.uniform(jax.random.fold_in(jax.random.fold_in(own_key, 6), dim), (shards_of,), jnp.float32, least / len(pieces), top_value / len(pieces))
        return jnp.repeat(jnp.exp(heights), extent[dim] // shards_of).reshape((-1,) + (1,) * (len(extent) - dim - 1))

    gain = one(*pieces[0])
    for cut in pieces[1:]:
        gain = gain * one(*cut)
    return gain


def gaussian(rng, dims, deviation, reach, pieces=(), kind=jnp.bfloat16):
    level = level_of(rng, dims, pieces, -0.22, 0.18) if pieces else 1.0
    drawn = jax.random.normal(rng, dims, jnp.float32) * deviation * level
    return jnp.minimum(jnp.maximum(drawn, -reach), reach).astype(kind)


def setup_inputs(seed: int = 0) -> dict:
    streams_of = jax.random.split(jax.random.key(seed), 9)
    queries = draw_queries(jax.random.fold_in(streams_of[8], 71), 0)
    keys_new = draw_keys_new(jax.random.fold_in(streams_of[8], 71), 0)
    values_new = gaussian(streams_of[2], (ROWS, KV_HEADS * HEAD), 1.0, 6.0, ((0, 8), (1, 4)))
    caches = gaussian(streams_of[3], (N_REP * SLOTS, 2, CACHE, KV_HEADS * HEAD), 1.0, 6.0, ((0, 8), (3, 4)))
    lengths = draw_lengths(jax.random.fold_in(streams_of[8], 71), 0)
    moving = with_ends(jax.random.randint(streams_of[5], (N_REP,), 0, SLOTS), jax.random.fold_in(streams_of[5], 1), 0, SLOTS - 1).astype(jnp.int32)
    destination = jax.random.permutation(streams_of[6], N_REP).astype(jnp.int32)
    out_weight = gaussian(streams_of[7], (HEADS * HEAD, OUT), (HEADS * HEAD) ** -0.5, 0.09375, ((0, 4),))
    return {"queries": queries, "keys_new": keys_new, "values_new": values_new, "caches": caches, "lengths": lengths, "moving": moving, "destination": destination, "out_weight": out_weight}


masked_score = -1e30
key_block_rows = 512


def product(form, left, right):
    return jnp.einsum(form, left.astype(jnp.float32), right.astype(jnp.float32))


def attend(query_slot, key_cache, value_cache, length, keys_fresh, values_fresh, block_count):
    span_rows = query_slot.shape[0]
    kv_count = key_cache.shape[1] // HEAD
    group_size = query_slot.shape[1] // (HEAD * kv_count)
    grouped = query_slot.reshape(span_rows, kv_count, group_size, HEAD).transpose(1, 2, 0, 3)
    grouped = grouped.reshape(kv_count, group_size * span_rows, HEAD)
    scale = HEAD ** -0.5
    token_of_row = jnp.arange(group_size * span_rows, dtype=jnp.int32) % span_rows

    def absorb(running, key_block, value_block, visible):
        row_max, row_total, weighted = running
        scores = product('gqd,kgd->gqk', grouped, key_block) * scale
        scores = jnp.where(visible, scores, masked_score)
        new_max = jnp.maximum(row_max, jnp.max(scores, axis=2))
        rescale = jnp.exp(row_max - new_max)
        weights_block = jnp.where(visible, jnp.exp(scores - new_max[:, :, None]), 0.0)
        row_total = row_total * rescale + jnp.sum(weights_block, axis=2)
        rounded = lax.optimization_barrier(weights_block.astype(jnp.bfloat16))
        weighted = weighted * rescale[:, :, None] + product('gqk,kgd->gqd', rounded, value_block)
        return new_max, row_total, weighted

    def cache_step(block_index, running):
        start = block_index * key_block_rows
        key_block = lax.dynamic_slice_in_dim(key_cache, start, key_block_rows, 0).reshape(key_block_rows, kv_count, HEAD)
        value_block = lax.dynamic_slice_in_dim(value_cache, start, key_block_rows, 0).reshape(key_block_rows, kv_count, HEAD)
        visible = (start + jnp.arange(key_block_rows, dtype=jnp.int32) < length)[None, None, :]
        return absorb(running, key_block, value_block, visible)

    rows_all = group_size * span_rows
    initial = (jnp.full((kv_count, rows_all), masked_score, jnp.float32),
               jnp.zeros((kv_count, rows_all), jnp.float32),
               jnp.zeros((kv_count, rows_all, HEAD), jnp.float32))
    running = lax.fori_loop(0, block_count, cache_step, initial)
    visible = (jnp.arange(span_rows, dtype=jnp.int32)[None, :] <= token_of_row[:, None])[None]
    running = absorb(running, keys_fresh.reshape(span_rows, kv_count, HEAD),
                     values_fresh.reshape(span_rows, kv_count, HEAD), visible)
    result = running[2] / running[1][:, :, None]
    result = result.reshape(kv_count, group_size, span_rows, HEAD).transpose(2, 0, 1, 3)
    return result.reshape(span_rows, kv_count * group_size * HEAD).astype(jnp.bfloat16)


def reference(queries, keys_new, values_new, caches, lengths, moving, destination, out_weight):
    source_of = jnp.argsort(destination).astype(jnp.int32)
    flat_lengths = lengths.reshape(-1)
    slot_indices = jnp.arange(N_REP * SLOTS, dtype=jnp.int32)
    replica_of = slot_indices // SLOTS
    number_of = slot_indices % SLOTS
    anchor_of = source_of[replica_of]
    taken_all = jnp.where(number_of == moving[replica_of], anchor_of * SLOTS + moving[anchor_of],
                          slot_indices).astype(jnp.int32)
    held_cache = jnp.take(caches, taken_all, axis=0)

    def per_slot(slot_index):
        taken = taken_all[slot_index]
        cache_slot = lax.dynamic_index_in_dim(held_cache, slot_index, 0, keepdims=False)
        length = flat_lengths[taken]
        start = (slot_index * SPAN).astype(jnp.int32)
        query_slot = lax.dynamic_slice_in_dim(queries, start, SPAN, 0)
        keys_fresh = lax.dynamic_slice_in_dim(keys_new, start, SPAN, 0)
        values_fresh = lax.dynamic_slice_in_dim(values_new, start, SPAN, 0)
        return attend(query_slot, cache_slot[0], cache_slot[1], length, keys_fresh, values_fresh, CACHE // key_block_rows)

    attended = lax.map(per_slot, slot_indices)
    attended = attended.reshape(N_REP * SLOTS * SPAN, HEADS * HEAD)
    mixed = jnp.dot(attended, out_weight, preferred_element_type=jnp.float32).astype(jnp.bfloat16)
    return (mixed, held_cache)
```

```python
import functools
import itertools
import random

import jax
import jax.numpy as jnp
import numpy as np
from jax import lax
from jax.experimental import pallas as pl
from jax.experimental.pallas import tpu as pltpu
from jax.sharding import PartitionSpec as P

HEAD = 128
BLOCK = 512
LOG2E = 1.4426950408889634
masked_score = -1e30
BLOCK_ROWS = 64


def slot_kernel(
    scalars, source, query_t, keys_fresh, values_fresh, *rest, aliased, kv_count, group
):
    if aliased:
        rest = rest[1:]
    held, attended, cache, row_max, row_total, weighted, in_sem, out_sem = rest
    taken, target, length = scalars[0], scalars[1], scalars[2]
    rows = cache.shape[1]
    blocks = rows // BLOCK
    span = keys_fresh.shape[0]
    factor = HEAD ** (-0.5) * LOG2E

    def fetch(block, part):
        at = pl.ds(pl.multiple_of(block * BLOCK, BLOCK), BLOCK)
        return pltpu.make_async_copy(
            source.at[taken, part, at], cache.at[part, at], in_sem.at[block, part]
        )

    def put(block, part):
        at = pl.ds(pl.multiple_of(block * BLOCK, BLOCK), BLOCK)
        return pltpu.make_async_copy(
            cache.at[part, at], held.at[target, part, at], out_sem.at[block, part]
        )

    for block in range(blocks):
        for part in range(2):
            fetch(block, part).start()

    def scores_of(head, keys):
        return lax.dot_general(
            keys,
            query_t[head],
            (((1,), (0,)), ((), ())),
            preferred_element_type=jnp.float32,
        )

    def mix(values, weights):
        return lax.dot_general(
            values,
            weights.astype(jnp.bfloat16),
            (((0,), (0,)), ((), ())),
            preferred_element_type=jnp.float32,
        )

    key_at = lax.broadcasted_iota(jnp.int32, (span, group * span), 0)
    token_at = lax.broadcasted_iota(jnp.int32, (span, group * span), 1) % span
    for head in range(kv_count):
        lanes = slice(head * HEAD, (head + 1) * HEAD)
        scores = jnp.where(
            key_at <= token_at, scores_of(head, keys_fresh[:, lanes]), masked_score
        )
        new_max = jnp.max(scores, axis=0, keepdims=True)
        weights = jnp.exp2((scores - new_max) * factor)
        row_max[head] = new_max
        row_total[head] = jnp.sum(weights, axis=0, keepdims=True)
        weighted[head] = mix(values_fresh[:, lanes], weights)

    def absorb(block, masked):
        start = pl.multiple_of(block * BLOCK, BLOCK)
        at = pl.ds(start, BLOCK)
        for head in range(kv_count):
            lanes = slice(head * HEAD, (head + 1) * HEAD)
            scores = scores_of(head, cache[0, at, lanes])
            if masked:
                position = start + lax.broadcasted_iota(jnp.int32, scores.shape, 0)
                scores = jnp.where(position < length, scores, masked_score)
            old_max = row_max[head]
            new_max = jnp.maximum(old_max, jnp.max(scores, axis=0, keepdims=True))
            rescale = jnp.exp2((old_max - new_max) * factor)
            weights = jnp.exp2((scores - new_max) * factor)
            row_max[head] = new_max
            row_total[head] = row_total[head] * rescale + jnp.sum(
                weights, axis=0, keepdims=True
            )
            weighted[head] = weighted[head] * rescale + mix(cache[1, at, lanes], weights)

    def step(block, carry):
        for part in range(2):
            fetch(block, part).wait()
            put(block, part).start()
        start = block * BLOCK

        @pl.when(start + BLOCK <= length)
        def _():
            absorb(block, False)

        @pl.when((start < length) & (length < start + BLOCK))
        def _():
            absorb(block, True)

        return carry

    lax.fori_loop(0, blocks, step, 0)
    for head in range(kv_count):
        result = (weighted[head] / row_total[head]).T
        for member in range(group):
            lanes = slice((head * group + member) * HEAD, (head * group + member + 1) * HEAD)
            attended[:, lanes] = result[member * span : (member + 1) * span].astype(
                jnp.bfloat16
            )
    for block in range(blocks):
        for part in range(2):
            put(block, part).wait()


def attend_slot(scalars, source, query_t, keys_fresh, values_fresh, held, held_shape):
    kv_count, _, columns = query_t.shape
    span = keys_fresh.shape[0]
    group = columns // span
    rows, width = source.shape[2:]
    aliased = held is not None
    anywhere = pl.BlockSpec(memory_space=pl.ANY)
    vmem = pl.BlockSpec(memory_space=pltpu.VMEM)
    operands = [scalars, source, query_t, keys_fresh, values_fresh]
    in_specs = [pl.BlockSpec(memory_space=pltpu.SMEM), anywhere, vmem, vmem, vmem]
    if aliased:
        operands.append(held)
        in_specs.append(anywhere)
    blocks = rows // BLOCK
    return pl.pallas_call(
        functools.partial(slot_kernel, aliased=aliased, kv_count=kv_count, group=group),
        out_shape=(
            jax.ShapeDtypeStruct(held_shape, jnp.bfloat16),
            jax.ShapeDtypeStruct((span, kv_count * group * HEAD), jnp.bfloat16),
        ),
        in_specs=in_specs,
        out_specs=(anywhere, vmem),
        scratch_shapes=[
            pltpu.VMEM((2, rows, width), jnp.bfloat16),
            pltpu.VMEM((kv_count, 1, columns), jnp.float32),
            pltpu.VMEM((kv_count, 1, columns), jnp.float32),
            pltpu.VMEM((kv_count, HEAD, columns), jnp.float32),
            pltpu.SemaphoreType.DMA((blocks, 2)),
            pltpu.SemaphoreType.DMA((blocks, 2)),
        ],
        input_output_aliases={5: 0} if aliased else {},
        compiler_params=pltpu.CompilerParams(vmem_limit_bytes=60 * 1024 * 1024),
        cost_estimate=pl.CostEstimate(
            flops=4 * kv_count * columns * (rows + span) * HEAD,
            bytes_accessed=8 * rows * width,
            transcendentals=kv_count * columns * (rows + span),
        ),
    )(*operands)


def project_kernel(
    attended, weight, out, weight_blocks, outgoing, incoming, weight_sem, send_sem, recv_sem
):
    parts = weight_blocks.shape[0]
    own = lax.axis_index("tp")
    columns = out.shape[1]

    def load(step):
        part = lax.rem(own + step, parts)
        at = pl.ds(pl.multiple_of(part * columns, columns), columns)
        return pltpu.make_async_copy(
            weight.at[:, at], weight_blocks.at[step], weight_sem.at[step]
        )

    order = list(range(1, parts)) + [0]
    for step in order:
        load(step).start()
    barrier = pltpu.get_barrier_semaphore()
    for step in range(1, parts):
        pl.semaphore_signal(
            barrier,
            inc=1,
            device_id={"tp": lax.rem(own + step, parts)},
            device_id_type=pl.DeviceIdType.MESH,
        )

    def product(step):
        load(step).wait()
        return jnp.dot(
            attended[...], weight_blocks[step], preferred_element_type=jnp.float32
        )

    copies = []
    for step in range(1, parts):
        outgoing[step - 1] = product(step).astype(jnp.bfloat16)
        if step == 1:
            pl.semaphore_wait(barrier, parts - 1)
        copy = pltpu.make_async_remote_copy(
            src_ref=outgoing.at[step - 1],
            dst_ref=incoming.at[step - 1],
            send_sem=send_sem.at[step - 1],
            recv_sem=recv_sem.at[step - 1],
            device_id={"tp": lax.rem(own + step, parts)},
            device_id_type=pl.DeviceIdType.MESH,
        )
        copy.start()
        copies.append(copy)
    total = product(0)
    for step, copy in enumerate(copies):
        copy.wait_recv()
        total = total + incoming[step].astype(jnp.float32)
    out[...] = total.astype(jnp.bfloat16)
    for copy in copies:
        copy.wait_send()


def project(attended, out_weight, identity):
    parts = lax.axis_size("tp")
    rows, depth = attended.shape
    columns = out_weight.shape[1] // parts
    vmem = pl.BlockSpec(memory_space=pltpu.VMEM)
    return pl.pallas_call(
        project_kernel,
        out_shape=jax.ShapeDtypeStruct((rows, columns), jnp.bfloat16),
        in_specs=[vmem, pl.BlockSpec(memory_space=pl.ANY)],
        out_specs=vmem,
        scratch_shapes=[
            pltpu.VMEM((parts, depth, columns), jnp.bfloat16),
            pltpu.VMEM((parts - 1, rows, columns), jnp.bfloat16),
            pltpu.VMEM((parts - 1, rows, columns), jnp.bfloat16),
            pltpu.SemaphoreType.DMA((parts,)),
            pltpu.SemaphoreType.DMA((parts - 1,)),
            pltpu.SemaphoreType.DMA((parts - 1,)),
        ],
        compiler_params=pltpu.CompilerParams(
            collective_id=identity, has_side_effects=True, vmem_limit_bytes=60 * 1024 * 1024
        ),
        cost_estimate=pl.CostEstimate(
            flops=2 * rows * depth * columns * parts,
            bytes_accessed=2 * depth * columns * parts,
            transcendentals=0,
        ),
        name=f"project{identity}",
    )(attended, out_weight)


QUARTERS = 4
STREAMS = 4


def cut_bound(held_at):
    chips = range(4)
    loads = []
    for bit in (1, 2):
        for side in (0, bit):
            loads.append(
                sum(
                    held_at[c][d]
                    for c in chips
                    for d in chips
                    if c & bit == side and d & bit != side
                )
            )
    for c in chips:
        loads.append(sum(held_at[c][d] for d in chips if d != c))
        loads.append(sum(held_at[d][c] for d in chips if d != c))
    return max(-(-load // 2) for load in loads)


def left_hops(held_at):
    return sum(
        held_at[c][d] * (((c ^ d) & 1) + ((c ^ d) >> 1)) for c in range(4) for d in range(4)
    )


def try_moves(held_at, slots, rng, noise):
    held_at = [row[:] for row in held_at]
    moves = []
    for slot in range(slots):
        left = slots - slot
        hops = left_hops(held_at)
        if hops == 0:
            moves.append({})
            continue
        if hops > 8 * left or cut_bound(held_at) > left:
            return None
        free = [row[:] for row in held_at]
        chosen = {}
        links = [(c, link) for c in range(4) for link in (1, 2)]
        rng.shuffle(links)
        for c, link in links:
            best = None
            for d in range(4):
                if free[c][d] <= 0 or c == d:
                    continue
                if (c ^ d) == 3:
                    value = 2.0 + noise * rng.random()
                elif (c ^ d) & link:
                    value = 1.5 + 0.1 * free[c][d] + noise * rng.random()
                elif left >= 3 and free[c][d] > left - 1:
                    value = 0.5 + 1.5 * noise * rng.random()
                else:
                    continue
                if best is None or value > best[0]:
                    best = (value, d)
            if best:
                chosen[c, link] = best[1]
                free[c][best[1]] -= 1
        for (c, link), d in chosen.items():
            held_at[c][d] -= 1
            held_at[c ^ link][d] += 1
        moves.append(chosen)
    return moves if left_hops(held_at) == 0 else None


def find_moves(demand, rng, most):
    held_at = [[0] * 4 for _ in range(4)]
    for c in range(4):
        for d in demand[c]:
            held_at[c][d] += QUARTERS
    least = max(cut_bound(held_at), -(-left_hops(held_at) // 8))
    for slots in range(least, most + 1):
        for attempt in range(400):
            noise = 0.0 if attempt == 0 else (0.5 if attempt % 2 else 1.5)
            moves = try_moves(held_at, slots, rng, noise)
            if moves is not None:
                return slots, moves
    raise ValueError("no route")


def codes_of(demand, moves, most):
    ready = [[[] for _ in range(4)] for _ in range(4)]
    arriving = []
    for c in range(4):
        for place, d in enumerate(demand[c]):
            for k in range(QUARTERS):
                ready[c][d].append((place * QUARTERS + k, (c, place, k)))
    send = [[[0] * most for _ in range(2)] for _ in range(4)]
    for slot, chosen in enumerate(moves):
        arriving = []
        for (c, link), d in sorted(chosen.items()):
            code, chunk = ready[c][d].pop(0)
            send[c][link - 1][slot] = code
            arriving.append((c ^ link, d, 2 * QUARTERS + 2 * slot + link - 1, chunk))
        for c, d, code, chunk in arriving:
            ready[c][d].append((code, chunk))
    table = []
    for c in range(4):
        here = {chunk: code for code, chunk in ready[c][c]}
        items = sorted({chunk[:2] for chunk in here})
        finals = [here[item + (k,)] for item in items for k in range(QUARTERS)]
        table.append(send[c][0] + send[c][1] + finals)
    return table


@functools.lru_cache
def routes(most):
    pairs = [(a, b) for a in range(4) for b in range(a, 4)]
    rng = random.Random(1)
    place = np.zeros((len(pairs) ** 4,), np.int32)
    rows, slots = [], []
    for index, demand in enumerate(itertools.product(pairs, repeat=4)):
        flat = [d for pair in demand for d in pair]
        if any(flat.count(d) != 2 for d in range(4)):
            continue
        place[index] = len(rows)
        count, moves = find_moves(demand, rng, most)
        rows.append(codes_of(demand, moves, most))
        slots.append(count)
    return place, np.array(rows, np.int32), np.array(slots, np.int32)


def plan_routes(destination, source_of, own, counts):
    place, rows, slots = routes(counts[-1])
    chip = own // 2
    first, second = destination[0::2] // 2, destination[1::2] // 2
    low, high = jnp.minimum(first, second), jnp.maximum(first, second)
    pair = low * (7 - low) // 2 + high
    key = jnp.sum(pair * jnp.array([1000, 100, 10, 1], jnp.int32))
    row = jnp.asarray(place)[key]
    codes = jnp.asarray(rows)[row, chip]
    swap = (first > second)[chip]
    local = codes < 2 * QUARTERS
    codes = jnp.where(local & swap, (codes + QUARTERS) % (2 * QUARTERS), codes)
    finals = codes[2 * counts[-1] :]
    crossed = source_of[2 * chip] > source_of[2 * chip + 1]
    finals = jnp.where(crossed, jnp.roll(finals, QUARTERS), finals)
    variant = jnp.sum(jnp.asarray(slots)[row] > jnp.array(counts[:-1], jnp.int32))
    return jnp.concatenate([codes[: 2 * counts[-1]], finals]), variant


def route_kernel(
    plan, attended, caches, weight, arrived, mixed, *rest, slots, most
):
    both, rest = rest[:STREAMS], rest[STREAMS:]
    local, rest = rest[:STREAMS], rest[STREAMS:]
    give, arr, stage, keep, hand, weight_blocks, outgoing, incoming, *sems = rest
    in_sem, give_sem, gave_sem, send_sem, recv_sem, keep_sem, hand_sem, got_sem, weight_sem, out_sem, mix_sem = sems
    own = lax.axis_index("rep")
    part = lax.axis_index("tp")
    parts = weight_blocks.shape[0]
    core = own % 2
    partner = own + 1 - 2 * core
    across = (own + 2 - 4 * ((own // 2) % 2), own + 4 - 8 * ((own // 4) % 2))
    rows = stage.shape[3]
    columns = mixed.shape[1]
    run = QUARTERS * rows
    leaving = plan[0]

    def fetch(s):
        return pltpu.make_async_copy(
            caches.at[:, :, pl.ds(s * run, run)], both[s], in_sem.at[s]
        )

    def load(step):
        at = pl.ds(pl.multiple_of(lax.rem(part + step, parts) * columns, columns), columns)
        return pltpu.make_async_copy(
            weight.at[:, at], weight_blocks.at[step], weight_sem.at[step]
        )

    for s in range(STREAMS):
        fetch(s).start()
    barrier = pltpu.get_barrier_semaphore()
    peers = [{"rep": partner}] + [{"rep": peer} for peer in across]
    peers += [{"tp": lax.rem(part + step, parts)} for step in range(1, parts)]
    for peer in peers:
        pl.semaphore_signal(
            barrier, inc=1, device_id=peer, device_id_type=pl.DeviceIdType.MESH
        )

    def remote(src, dst, send, recv, peer):
        return pltpu.make_async_remote_copy(
            src_ref=src,
            dst_ref=dst,
            send_sem=send,
            recv_sem=recv,
            device_id=peer,
            device_id_type=pl.DeviceIdType.MESH,
        )

    def share(s):
        return remote(
            give.at[s],
            local[s].at[pl.ds(core * QUARTERS, QUARTERS)],
            give_sem.at[s],
            gave_sem.at[s],
            {"rep": partner},
        )

    def send(link, slot, s):
        return remote(
            stage.at[link, slot, s],
            arr.at[link, slot, s],
            send_sem.at[link, slot, s],
            recv_sem.at[link, slot, s],
            {"rep": across[link]},
        )

    def settle(s):
        return pltpu.make_async_copy(
            keep.at[s], arrived.at[0, core, pl.ds(s * run, run)], keep_sem.at[s]
        )

    def deliver(s):
        return remote(
            hand.at[s],
            arrived.at[0, core, pl.ds(s * run, run)],
            hand_sem.at[s],
            got_sem.at[s],
            {"rep": partner},
        )

    def pick(s, upto, codes, write):
        homes = [jnp.minimum(code, 2 * QUARTERS - 1) for code in codes]

        def body(block, carry):
            at = pl.ds(pl.multiple_of(block * BLOCK_ROWS, BLOCK_ROWS), BLOCK_ROWS)
            values = [local[s][home, at] for home in homes]
            for slot in range(upto):
                for link in range(2):
                    code_here = 2 * QUARTERS + 2 * slot + link
                    came = arr[link, slot, s, at]
                    values = [
                        lax.select(code == code_here, came, value)
                        for code, value in zip(codes, values)
                    ]
            for index, value in enumerate(values):
                write(index, at, value)
            return carry

        lax.fori_loop(0, rows // BLOCK_ROWS, body, 0)

    for s in range(STREAMS):
        fetch(s).wait()
        for k in range(QUARTERS):
            def body(block, carry):
                inner = pl.multiple_of(block * BLOCK_ROWS, BLOCK_ROWS)
                at = pl.ds(k * rows + inner, BLOCK_ROWS)
                give[s, k, pl.ds(inner, BLOCK_ROWS)] = both[s][leaving, 1 - core, at]
                local[s][core * QUARTERS + k, pl.ds(inner, BLOCK_ROWS)] = both[s][
                    leaving, core, at
                ]
                return carry

            lax.fori_loop(0, rows // BLOCK_ROWS, body, 0)
        if s == 0:
            pl.semaphore_wait(barrier, len(peers))
        share(s).start()
    order = list(range(1, parts)) + [0]
    for step in order:
        load(step).start()

    def product(step):
        load(step).wait()
        return jnp.dot(
            attended[...], weight_blocks[step], preferred_element_type=jnp.float32
        )

    def mix(step):
        return remote(
            outgoing.at[step - 1],
            incoming.at[step - 1],
            out_sem.at[step - 1],
            mix_sem.at[step - 1],
            {"tp": lax.rem(part + step, parts)},
        )

    for slot in range(slots):
        for s in range(STREAMS):
            if slot == 0:
                share(s).wait_recv()
            else:
                for link in range(2):
                    send(link, slot - 1, s).wait_recv()
            codes = [plan[1 + link * most + slot] for link in range(2)]

            def write(link, at, value):
                stage[link, slot, s, at] = value

            pick(s, slot, codes, write)
            for link in range(2):
                send(link, slot, s).start()
        if 1 <= slot + 1 < parts:
            step = slot + 1
            outgoing[step - 1] = product(step).astype(jnp.bfloat16)
            mix(step).start()
    total = product(0)
    for s in range(STREAMS):
        for link in range(2):
            send(link, slots - 1, s).wait_recv()
        for k in range(QUARTERS):
            base = 1 + 2 * most + k
            codes = [plan[base + QUARTERS * core], plan[base + QUARTERS * (1 - core)]]

            def write(index, at, value):
                if index == 0:
                    keep[s, pl.ds(k * rows + at.start, BLOCK_ROWS)] = value
                else:
                    hand[s, pl.ds(k * rows + at.start, BLOCK_ROWS)] = value

            pick(s, slots, codes, write)
        settle(s).start()
        deliver(s).start()
    for step in range(1, parts):
        mix(step).wait_recv()
        total = total + incoming[step - 1].astype(jnp.float32)
    mixed[...] = total.astype(jnp.bfloat16)
    for step in range(1, parts):
        mix(step).wait_send()
    for s in range(STREAMS):
        share(s).wait_send()
        for slot in range(slots):
            for link in range(2):
                send(link, slot, s).wait_send()
        settle(s).wait()
        deliver(s).wait()


def route(plan, attended, caches, out_weight, slots, most, identity):
    parts = lax.axis_size("tp")
    span, depth = attended.shape
    columns = out_weight.shape[1] // parts
    slot_count, halves, cache_rows, width = caches.shape
    run = cache_rows // STREAMS
    rows = run // QUARTERS
    anywhere = pl.BlockSpec(memory_space=pl.ANY)
    vmem = pl.BlockSpec(memory_space=pltpu.VMEM)
    kind = jnp.bfloat16
    dma = pltpu.SemaphoreType.DMA
    scratch = [pltpu.VMEM((slot_count, halves, run, width), kind) for _ in range(STREAMS)]
    scratch += [pltpu.VMEM((2 * QUARTERS, rows, width), kind) for _ in range(STREAMS)]
    scratch += [
        pltpu.VMEM((STREAMS, QUARTERS, rows, width), kind),
        pltpu.VMEM((2, slots, STREAMS, rows, width), kind),
        pltpu.VMEM((2, slots, STREAMS, rows, width), kind),
        pltpu.VMEM((STREAMS, run, width), kind),
        pltpu.VMEM((STREAMS, run, width), kind),
        pltpu.VMEM((parts, depth, columns), kind),
        pltpu.VMEM((parts - 1, span, columns), kind),
        pltpu.VMEM((parts - 1, span, columns), kind),
        dma((STREAMS,)),
        dma((STREAMS,)),
        dma((STREAMS,)),
        dma((2, slots, STREAMS)),
        dma((2, slots, STREAMS)),
        dma((STREAMS,)),
        dma((STREAMS,)),
        dma((STREAMS,)),
        dma((parts,)),
        dma((parts - 1,)),
        dma((parts - 1,)),
    ]
    return pl.pallas_call(
        functools.partial(route_kernel, slots=slots, most=most),
        out_shape=(
            jax.ShapeDtypeStruct((1, halves, cache_rows, width), kind),
            jax.ShapeDtypeStruct((span, columns), kind),
        ),
        in_specs=[pl.BlockSpec(memory_space=pltpu.SMEM), vmem, anywhere, anywhere],
        out_specs=(anywhere, vmem),
        scratch_shapes=scratch,
        compiler_params=pltpu.CompilerParams(
            collective_id=identity, has_side_effects=True, vmem_limit_bytes=60 * 1024 * 1024
        ),
        name=f"route{slots}",
    )(plan, attended, caches, out_weight)


def on_device(queries, keys_new, values_new, caches, lengths, moving, destination, out_weight):
    replicas = lax.axis_size("rep")
    own_index = lax.axis_index("rep")
    slot_count, _, cache_rows, width = caches.shape
    span = queries.shape[0] // slot_count
    kv_count = width // HEAD
    group = queries.shape[1] // width
    leaving_slot = moving[own_index]
    staying_slot = 1 - leaving_slot
    every = jnp.arange(replicas, dtype=jnp.int32)
    source_of = jnp.sum(
        jnp.where(destination[None, :] == every[:, None], every[None, :], 0), axis=1
    )
    anchor = source_of[own_index]
    incoming_length = lengths[anchor, moving[anchor]]
    staying_length = lengths[own_index, staying_slot]
    query_t = (
        queries.reshape(slot_count, span, kv_count, group, HEAD)
        .transpose(0, 2, 4, 3, 1)
        .reshape(slot_count, kv_count, HEAD, group * span)
    )
    keys_by_slot = keys_new.reshape(slot_count, span, width)
    values_by_slot = values_new.reshape(slot_count, span, width)

    def pick(array, slot):
        return lax.dynamic_index_in_dim(array, slot, 0, keepdims=False)

    held, staying_attended = attend_slot(
        jnp.stack([staying_slot, staying_slot, staying_length]),
        caches,
        pick(query_t, staying_slot),
        pick(keys_by_slot, staying_slot),
        pick(values_by_slot, staying_slot),
        None,
        caches.shape,
    )
    if replicas == 8:
        counts = (6, 8)
        codes, variant = plan_routes(destination, source_of, own_index, counts)
        plan = jnp.concatenate([leaving_slot[None], codes])
        arrived, staying_mixed = lax.switch(
            variant,
            [
                functools.partial(route, slots=slots, most=counts[-1], identity=2 + index)
                for index, slots in enumerate(counts)
            ],
            plan,
            staying_attended,
            caches,
            out_weight,
        )
    else:
        leaving = lax.dynamic_index_in_dim(caches, leaving_slot, 0, keepdims=False)
        piece_rows = 2 * cache_rows // replicas
        pieces = leaving.reshape(replicas, piece_rows, width)
        spread = lax.all_to_all(pieces, "rep", split_axis=0, concat_axis=0, tiled=True)
        ordered = jnp.take(spread, source_of, axis=0, mode="clip")
        arrived = lax.all_to_all(ordered, "rep", split_axis=0, concat_axis=0, tiled=True)
        arrived = arrived.reshape(1, 2, cache_rows, width)
        staying_mixed = project(staying_attended, out_weight, 0)
    held, arrived_attended = attend_slot(
        jnp.stack([jnp.zeros_like(leaving_slot), leaving_slot, incoming_length]),
        arrived,
        pick(query_t, leaving_slot),
        pick(keys_by_slot, leaving_slot),
        pick(values_by_slot, leaving_slot),
        held,
        caches.shape,
    )
    arrived_mixed = project(arrived_attended, out_weight, 1)
    mixed = jnp.where(
        leaving_slot == 0,
        jnp.concatenate([arrived_mixed, staying_mixed], axis=0),
        jnp.concatenate([staying_mixed, arrived_mixed], axis=0),
    )
    return (mixed, held)


def solution(mesh):
    in_specs = (
        P("rep", "tp"),
        P("rep", "tp"),
        P("rep", "tp"),
        P("rep", None, None, "tp"),
        P(),
        P(),
        P(),
        P("tp", None),
    )
    out_specs = (P("rep", "tp"), P("rep", None, None, "tp"))
    return jax.shard_map(
        on_device, mesh=mesh, in_specs=in_specs, out_specs=out_specs, check_vma=False
    )
```

```python
import functools
import itertools
import random

import jax
import jax.numpy as jnp
import numpy as np
from jax import lax
from jax.experimental import pallas as pl
from jax.experimental.pallas import tpu as pltpu
from jax.sharding import PartitionSpec as P

HEAD = 128
BLOCK = 512
LOG2E = 1.4426950408889634
masked_score = -1e30
BLOCK_ROWS = 64


def slot_kernel(
    scalars, source, query_t, keys_fresh, values_fresh, *rest, aliased, kv_count, group
):
    if aliased:
        rest = rest[1:]
    held, attended, cache, row_max, row_total, weighted, in_sem, out_sem = rest
    taken, target, length = scalars[0], scalars[1], scalars[2]
    rows = cache.shape[1]
    blocks = rows // BLOCK
    span = keys_fresh.shape[0]
    factor = HEAD ** (-0.5) * LOG2E

    def fetch(block, part):
        at = pl.ds(pl.multiple_of(block * BLOCK, BLOCK), BLOCK)
        return pltpu.make_async_copy(
            source.at[taken, part, at], cache.at[part, at], in_sem.at[block, part]
        )

    def put(block, part):
        at = pl.ds(pl.multiple_of(block * BLOCK, BLOCK), BLOCK)
        return pltpu.make_async_copy(
            cache.at[part, at], held.at[target, part, at], out_sem.at[block, part]
        )

    for block in range(blocks):
        for part in range(2):
            fetch(block, part).start()

    def scores_of(head, keys):
        return lax.dot_general(
            keys,
            query_t[head],
            (((1,), (0,)), ((), ())),
            preferred_element_type=jnp.float32,
        )

    def mix(values, weights):
        return lax.dot_general(
            values,
            weights.astype(jnp.bfloat16),
            (((0,), (0,)), ((), ())),
            preferred_element_type=jnp.float32,
        )

    key_at = lax.broadcasted_iota(jnp.int32, (span, group * span), 0)
    token_at = lax.broadcasted_iota(jnp.int32, (span, group * span), 1) % span
    for head in range(kv_count):
        lanes = slice(head * HEAD, (head + 1) * HEAD)
        scores = jnp.where(
            key_at <= token_at, scores_of(head, keys_fresh[:, lanes]), masked_score
        )
        new_max = jnp.max(scores, axis=0, keepdims=True)
        weights = jnp.exp2((scores - new_max) * factor)
        row_max[head] = new_max
        row_total[head] = jnp.sum(weights, axis=0, keepdims=True)
        weighted[head] = mix(values_fresh[:, lanes], weights)

    def absorb(block, masked):
        start = pl.multiple_of(block * BLOCK, BLOCK)
        at = pl.ds(start, BLOCK)
        for head in range(kv_count):
            lanes = slice(head * HEAD, (head + 1) * HEAD)
            scores = scores_of(head, cache[0, at, lanes])
            if masked:
                position = start + lax.broadcasted_iota(jnp.int32, scores.shape, 0)
                scores = jnp.where(position < length, scores, masked_score)
            old_max = row_max[head]
            new_max = jnp.maximum(old_max, jnp.max(scores, axis=0, keepdims=True))
            rescale = jnp.exp2((old_max - new_max) * factor)
            weights = jnp.exp2((scores - new_max) * factor)
            row_max[head] = new_max
            row_total[head] = row_total[head] * rescale + jnp.sum(
                weights, axis=0, keepdims=True
            )
            weighted[head] = weighted[head] * rescale + mix(cache[1, at, lanes], weights)

    def step(block, carry):
        for part in range(2):
            fetch(block, part).wait()
            put(block, part).start()
        start = block * BLOCK

        @pl.when(start + BLOCK <= length)
        def _():
            absorb(block, False)

        @pl.when((start < length) & (length < start + BLOCK))
        def _():
            absorb(block, True)

        return carry

    lax.fori_loop(0, blocks, step, 0)
    for head in range(kv_count):
        result = (weighted[head] / row_total[head]).T
        for member in range(group):
            lanes = slice((head * group + member) * HEAD, (head * group + member + 1) * HEAD)
            attended[:, lanes] = result[member * span : (member + 1) * span].astype(
                jnp.bfloat16
            )
    for block in range(blocks):
        for part in range(2):
            put(block, part).wait()


def attend_slot(scalars, source, query_t, keys_fresh, values_fresh, held, held_shape):
    kv_count, _, columns = query_t.shape
    span = keys_fresh.shape[0]
    group = columns // span
    rows, width = source.shape[2:]
    aliased = held is not None
    anywhere = pl.BlockSpec(memory_space=pl.ANY)
    vmem = pl.BlockSpec(memory_space=pltpu.VMEM)
    operands = [scalars, source, query_t, keys_fresh, values_fresh]
    in_specs = [pl.BlockSpec(memory_space=pltpu.SMEM), anywhere, vmem, vmem, vmem]
    if aliased:
        operands.append(held)
        in_specs.append(anywhere)
    blocks = rows // BLOCK
    return pl.pallas_call(
        functools.partial(slot_kernel, aliased=aliased, kv_count=kv_count, group=group),
        out_shape=(
            jax.ShapeDtypeStruct(held_shape, jnp.bfloat16),
            jax.ShapeDtypeStruct((span, kv_count * group * HEAD), jnp.bfloat16),
        ),
        in_specs=in_specs,
        out_specs=(anywhere, vmem),
        scratch_shapes=[
            pltpu.VMEM((2, rows, width), jnp.bfloat16),
            pltpu.VMEM((kv_count, 1, columns), jnp.float32),
            pltpu.VMEM((kv_count, 1, columns), jnp.float32),
            pltpu.VMEM((kv_count, HEAD, columns), jnp.float32),
            pltpu.SemaphoreType.DMA((blocks, 2)),
            pltpu.SemaphoreType.DMA((blocks, 2)),
        ],
        input_output_aliases={5: 0} if aliased else {},
        compiler_params=pltpu.CompilerParams(vmem_limit_bytes=60 * 1024 * 1024),
        cost_estimate=pl.CostEstimate(
            flops=4 * kv_count * columns * (rows + span) * HEAD,
            bytes_accessed=8 * rows * width,
            transcendentals=kv_count * columns * (rows + span),
        ),
    )(*operands)


def project_kernel(
    attended, weight, out, weight_blocks, outgoing, incoming, weight_sem, send_sem, recv_sem
):
    parts = weight_blocks.shape[0]
    own = lax.axis_index("tp")
    columns = out.shape[1]

    def load(step):
        part = lax.rem(own + step, parts)
        at = pl.ds(pl.multiple_of(part * columns, columns), columns)
        return pltpu.make_async_copy(
            weight.at[:, at], weight_blocks.at[step], weight_sem.at[step]
        )

    order = list(range(1, parts)) + [0]
    for step in order:
        load(step).start()
    barrier = pltpu.get_barrier_semaphore()
    for step in range(1, parts):
        pl.semaphore_signal(
            barrier,
            inc=1,
            device_id={"tp": lax.rem(own + step, parts)},
            device_id_type=pl.DeviceIdType.MESH,
        )

    def product(step):
        load(step).wait()
        return jnp.dot(
            attended[...], weight_blocks[step], preferred_element_type=jnp.float32
        )

    copies = []
    for step in range(1, parts):
        outgoing[step - 1] = product(step).astype(jnp.bfloat16)
        if step == 1:
            pl.semaphore_wait(barrier, parts - 1)
        copy = pltpu.make_async_remote_copy(
            src_ref=outgoing.at[step - 1],
            dst_ref=incoming.at[step - 1],
            send_sem=send_sem.at[step - 1],
            recv_sem=recv_sem.at[step - 1],
            device_id={"tp": lax.rem(own + step, parts)},
            device_id_type=pl.DeviceIdType.MESH,
        )
        copy.start()
        copies.append(copy)
    total = product(0)
    for step, copy in enumerate(copies):
        copy.wait_recv()
        total = total + incoming[step].astype(jnp.float32)
    out[...] = total.astype(jnp.bfloat16)
    for copy in copies:
        copy.wait_send()


def project(attended, out_weight, identity):
    parts = lax.axis_size("tp")
    rows, depth = attended.shape
    columns = out_weight.shape[1] // parts
    vmem = pl.BlockSpec(memory_space=pltpu.VMEM)
    return pl.pallas_call(
        project_kernel,
        out_shape=jax.ShapeDtypeStruct((rows, columns), jnp.bfloat16),
        in_specs=[vmem, pl.BlockSpec(memory_space=pl.ANY)],
        out_specs=vmem,
        scratch_shapes=[
            pltpu.VMEM((parts, depth, columns), jnp.bfloat16),
            pltpu.VMEM((parts - 1, rows, columns), jnp.bfloat16),
            pltpu.VMEM((parts - 1, rows, columns), jnp.bfloat16),
            pltpu.SemaphoreType.DMA((parts,)),
            pltpu.SemaphoreType.DMA((parts - 1,)),
            pltpu.SemaphoreType.DMA((parts - 1,)),
        ],
        compiler_params=pltpu.CompilerParams(
            collective_id=identity, has_side_effects=True, vmem_limit_bytes=60 * 1024 * 1024
        ),
        cost_estimate=pl.CostEstimate(
            flops=2 * rows * depth * columns * parts,
            bytes_accessed=2 * depth * columns * parts,
            transcendentals=0,
        ),
        name=f"project{identity}",
    )(attended, out_weight)


QUARTERS = 4
STREAMS = 4


def cut_bound(held_at):
    chips = range(4)
    loads = []
    for bit in (1, 2):
        for side in (0, bit):
            loads.append(
                sum(
                    held_at[c][d]
                    for c in chips
                    for d in chips
                    if c & bit == side and d & bit != side
                )
            )
    for c in chips:
        loads.append(sum(held_at[c][d] for d in chips if d != c))
        loads.append(sum(held_at[d][c] for d in chips if d != c))
    return max(-(-load // 2) for load in loads)


def left_hops(held_at):
    return sum(
        held_at[c][d] * (((c ^ d) & 1) + ((c ^ d) >> 1)) for c in range(4) for d in range(4)
    )


def try_moves(held_at, slots, rng, noise):
    held_at = [row[:] for row in held_at]
    moves = []
    for slot in range(slots):
        left = slots - slot
        hops = left_hops(held_at)
        if hops == 0:
            moves.append({})
            continue
        if hops > 8 * left or cut_bound(held_at) > left:
            return None
        free = [row[:] for row in held_at]
        chosen = {}
        links = [(c, link) for c in range(4) for link in (1, 2)]
        rng.shuffle(links)
        for c, link in links:
            best = None
            for d in range(4):
                if free[c][d] <= 0 or c == d:
                    continue
                if (c ^ d) == 3:
                    value = 2.0 + noise * rng.random()
                elif (c ^ d) & link:
                    value = 1.5 + 0.1 * free[c][d] + noise * rng.random()
                elif left >= 3 and free[c][d] > left - 1:
                    value = 0.5 + 1.5 * noise * rng.random()
                else:
                    continue
                if best is None or value > best[0]:
                    best = (value, d)
            if best:
                chosen[c, link] = best[1]
                free[c][best[1]] -= 1
        for (c, link), d in chosen.items():
            held_at[c][d] -= 1
            held_at[c ^ link][d] += 1
        moves.append(chosen)
    return moves if left_hops(held_at) == 0 else None


def find_moves(demand, rng, most):
    held_at = [[0] * 4 for _ in range(4)]
    for c in range(4):
        for d in demand[c]:
            held_at[c][d] += QUARTERS
    least = max(cut_bound(held_at), -(-left_hops(held_at) // 8))
    for slots in range(least, most + 1):
        for attempt in range(400):
            noise = 0.0 if attempt == 0 else (0.5 if attempt % 2 else 1.5)
            moves = try_moves(held_at, slots, rng, noise)
            if moves is not None:
                return slots, moves
    raise ValueError("no route")


def codes_of(demand, moves, most):
    ready = [[[] for _ in range(4)] for _ in range(4)]
    arriving = []
    for c in range(4):
        for place, d in enumerate(demand[c]):
            for k in range(QUARTERS):
                ready[c][d].append((place * QUARTERS + k, (c, place, k)))
    send = [[[0] * most for _ in range(2)] for _ in range(4)]
    for slot, chosen in enumerate(moves):
        arriving = []
        for (c, link), d in sorted(chosen.items()):
            code, chunk = ready[c][d].pop(0)
            send[c][link - 1][slot] = code
            arriving.append((c ^ link, d, 2 * QUARTERS + 2 * slot + link - 1, chunk))
        for c, d, code, chunk in arriving:
            ready[c][d].append((code, chunk))
    table = []
    for c in range(4):
        here = {chunk: code for code, chunk in ready[c][c]}
        items = sorted({chunk[:2] for chunk in here})
        finals = [here[item + (k,)] for item in items for k in range(QUARTERS)]
        table.append(send[c][0] + send[c][1] + finals)
    return table


@functools.lru_cache
def routes(most):
    pairs = [(a, b) for a in range(4) for b in range(a, 4)]
    rng = random.Random(1)
    place = np.zeros((len(pairs) ** 4,), np.int32)
    rows, slots = [], []
    for index, demand in enumerate(itertools.product(pairs, repeat=4)):
        flat = [d for pair in demand for d in pair]
        if any(flat.count(d) != 2 for d in range(4)):
            continue
        place[index] = len(rows)
        count, moves = find_moves(demand, rng, most)
        rows.append(codes_of(demand, moves, most))
        slots.append(count)
    return place, np.array(rows, np.int32), np.array(slots, np.int32)


def plan_kernel(lengths, moving, destination, place, rows, plan, found, line, sem, *, most):
    replicas = destination.shape[0]
    own = lax.axis_index("rep")
    chip = own // 2
    key = jnp.int32(0)
    swap = jnp.int32(0)
    for c in range(replicas // 2):
        first, second = destination[2 * c] // 2, destination[2 * c + 1] // 2
        low, high = jnp.minimum(first, second), jnp.maximum(first, second)
        key = key * 10 + low * (7 - low) // 2 + high
        swap = jnp.where(c == chip, (first > second).astype(jnp.int32), swap)
    seek = pltpu.make_async_copy(place.at[key // 128], found, sem)
    seek.start()
    anchor = jnp.int32(0)
    senders = [jnp.int32(0), jnp.int32(0)]
    for r in range(replicas):
        goal = destination[r]
        anchor = jnp.where(goal == own, r, anchor)
        senders = [
            jnp.where(goal == 2 * chip + index, r, sender)
            for index, sender in enumerate(senders)
        ]
    crossed = (senders[0] > senders[1]).astype(jnp.int32)
    leaving = moving[own]
    plan[0] = leaving
    plan[1] = lengths[own, 1 - leaving]
    plan[2] = lengths[anchor, moving[anchor]]
    seek.wait()
    fetch = pltpu.make_async_copy(rows.at[found[0, key % 128]], line, sem)
    fetch.start()
    fetch.wait()
    plan[3] = line[0, line.shape[1] - 1]
    size = 2 * most + 2 * QUARTERS
    for index in range(size):
        at = index
        if index >= 2 * most:
            final = index - 2 * most
            at = 2 * most + (final + QUARTERS * crossed) % (2 * QUARTERS)
        code = line[0, chip * size + at]
        turned = (code + QUARTERS * swap) % (2 * QUARTERS)
        plan[4 + index] = jnp.where(code < 2 * QUARTERS, turned, code)


def make_plan(lengths, moving, destination, counts):
    most = counts[-1]
    place, rows, slots = routes(most)
    lines = -(-place.size // 128)
    places = np.zeros((lines * 128,), np.int32)
    places[: place.size] = place
    table = np.zeros((rows.shape[0], 1, 128), np.int32)
    table[:, 0, : rows[0].size] = rows.reshape(rows.shape[0], -1)
    table[:, 0, 127] = np.sum(slots[:, None] > np.array(counts[:-1]), axis=1)
    anywhere = pl.BlockSpec(memory_space=pl.ANY)
    smem = pl.BlockSpec(memory_space=pltpu.SMEM)
    return pl.pallas_call(
        functools.partial(plan_kernel, most=most),
        out_shape=jax.ShapeDtypeStruct((4 + 2 * most + 2 * QUARTERS,), jnp.int32),
        in_specs=[smem, smem, smem, anywhere, anywhere],
        out_specs=smem,
        scratch_shapes=[
            pltpu.SMEM((1, 128), jnp.int32),
            pltpu.SMEM((1, 128), jnp.int32),
            pltpu.SemaphoreType.DMA,
        ],
        name="plan",
    )(lengths, moving, destination, jnp.asarray(places.reshape(lines, 1, 128)), jnp.asarray(table))


def route_kernel(
    plan,
    queries,
    keys_new,
    values_new,
    caches,
    weight,
    arrived,
    mixed,
    both,
    local,
    give,
    arr,
    stage,
    final,
    hand,
    query_t,
    row_max,
    row_total,
    weighted,
    attended,
    weight_blocks,
    outgoing,
    incoming,
    in_sem,
    give_sem,
    gave_sem,
    send_sem,
    recv_sem,
    keep_sem,
    hand_sem,
    got_sem,
    weight_sem,
    out_sem,
    mix_sem,
    *,
    slots,
    most,
):
    own = lax.axis_index("rep")
    part = lax.axis_index("tp")
    parts = weight_blocks.shape[0]
    core = own % 2
    partner = own + 1 - 2 * core
    across = (own + 2 - 4 * ((own // 2) % 2), own + 4 - 8 * (own // 4))
    rows = stage.shape[3]
    span, columns = mixed.shape[1:]
    kv_count = query_t.shape[0]
    group = query_t.shape[2] // span
    run = QUARTERS * rows
    factor = HEAD ** (-0.5) * LOG2E
    leaving = plan[0]

    def fetch(s):
        return pltpu.make_async_copy(
            caches.at[:, :, pl.ds(s * run, run)], both.at[s], in_sem.at[s]
        )

    def load(step):
        at = pl.ds(pl.multiple_of(lax.rem(part + step, parts) * columns, columns), columns)
        return pltpu.make_async_copy(
            weight.at[:, at], weight_blocks.at[step], weight_sem.at[step]
        )

    for s in range(STREAMS):
        fetch(s).start()
    barrier = pltpu.get_barrier_semaphore()
    peers = [{"rep": partner}] + [{"rep": peer} for peer in across]
    peers += [{"tp": lax.rem(part + step, parts)} for step in range(1, parts)]
    for peer in peers:
        pl.semaphore_signal(
            barrier, inc=1, device_id=peer, device_id_type=pl.DeviceIdType.MESH
        )

    def remote(src, dst, send, recv, peer):
        return pltpu.make_async_remote_copy(
            src_ref=src,
            dst_ref=dst,
            send_sem=send,
            recv_sem=recv,
            device_id=peer,
            device_id_type=pl.DeviceIdType.MESH,
        )

    def share(s):
        return remote(
            give.at[s],
            local.at[s, pl.ds(core * QUARTERS, QUARTERS)],
            give_sem.at[s],
            gave_sem.at[s],
            {"rep": partner},
        )

    def send(link, slot, s):
        return remote(
            stage.at[link, slot, s],
            arr.at[link, slot, s],
            send_sem.at[link, slot, s],
            recv_sem.at[link, slot, s],
            {"rep": across[link]},
        )

    def settle(s, half):
        return pltpu.make_async_copy(
            final.at[s, half],
            arrived.at[0, half, pl.ds(s * run, run)],
            keep_sem.at[s, half],
        )

    def deliver(s):
        return remote(
            hand.at[s],
            final.at[s, core],
            hand_sem.at[s],
            got_sem.at[s],
            {"rep": partner},
        )

    def mix(kind, step):
        return remote(
            outgoing.at[kind, step - 1],
            incoming.at[kind, step - 1],
            out_sem.at[kind, step - 1],
            mix_sem.at[kind, step - 1],
            {"tp": lax.rem(part + step, parts)},
        )

    def pick(s, upto, codes, write):
        def body(block, carry):
            at = pl.ds(pl.multiple_of(block * BLOCK_ROWS, BLOCK_ROWS), BLOCK_ROWS)
            values = [local[s, 0, at]] * len(codes)
            came = [(home, local[s, home, at]) for home in range(1, 2 * QUARTERS)]
            came += [
                (2 * QUARTERS + 2 * slot + link, arr[link, slot, s, at])
                for slot in range(upto)
                for link in range(2)
            ]
            for here, piece in came:
                values = [
                    lax.select(code == here, piece, value)
                    for code, value in zip(codes, values)
                ]
            for index, value in enumerate(values):
                write(index, block, value)
            return carry

        lax.fori_loop(0, rows // BLOCK_ROWS, body, 0)

    def share_out(s, carry):
        fetch(s).wait()

        def body(block, carry):
            k = block // (rows // BLOCK_ROWS)
            inner = pl.multiple_of(block % (rows // BLOCK_ROWS) * BLOCK_ROWS, BLOCK_ROWS)
            at = pl.ds(pl.multiple_of(block * BLOCK_ROWS, BLOCK_ROWS), BLOCK_ROWS)
            to = pl.ds(inner, BLOCK_ROWS)
            for half, into in ((1 - core, None), (core, core)):
                value = lax.select(
                    leaving == 0, both[s, 0, half, at], both[s, 1, half, at]
                )
                if into is None:
                    give[s, k, to] = value
                else:
                    local[s, core * QUARTERS + k, to] = value
            return carry

        lax.fori_loop(0, run // BLOCK_ROWS, body, 0)

        @pl.when(s == 0)
        def _():
            pl.semaphore_wait(barrier, len(peers))

        share(s).start()
        return carry

    lax.fori_loop(0, STREAMS, share_out, 0)
    for step in list(range(1, parts)) + [0]:
        load(step).start()

    def lanes_of(head):
        return slice(head * HEAD, (head + 1) * HEAD)

    def mix_values(values, weights):
        return lax.dot_general(
            values,
            weights.astype(jnp.bfloat16),
            (((0,), (0,)), ((), ())),
            preferred_element_type=jnp.float32,
        )

    def scores_of(head, keys):
        return lax.dot_general(
            keys,
            query_t[head],
            (((1,), (0,)), ((), ())),
            preferred_element_type=jnp.float32,
        )

    def fresh(slot):
        def choose(ref, lanes):
            return lax.select(slot == 0, ref[0, :, lanes], ref[1, :, lanes])

        key_at = lax.broadcasted_iota(jnp.int32, (span, group * span), 0)
        token_at = lax.broadcasted_iota(jnp.int32, (span, group * span), 1) % span
        for head in range(kv_count):
            for member in range(group):
                query_t[head, :, member * span : (member + 1) * span] = choose(
                    queries, lanes_of(head * group + member)
                ).T
            scores = jnp.where(
                key_at <= token_at, scores_of(head, choose(keys_new, lanes_of(head))), masked_score
            )
            new_max = jnp.max(scores, axis=0, keepdims=True)
            weights = jnp.exp2((scores - new_max) * factor)
            row_max[head] = new_max
            row_total[head] = jnp.sum(weights, axis=0, keepdims=True)
            weighted[head] = mix_values(choose(values_new, lanes_of(head)), weights)

    def absorb(start, length, piece):
        for head in range(kv_count):
            scores = scores_of(head, piece(0, head))
            position = start + lax.broadcasted_iota(jnp.int32, scores.shape, 0)
            scores = jnp.where(position < length, scores, masked_score)
            old_max = row_max[head]
            new_max = jnp.maximum(old_max, jnp.max(scores, axis=0, keepdims=True))
            rescale = jnp.exp2((old_max - new_max) * factor)
            weights = jnp.exp2((scores - new_max) * factor)
            row_max[head] = new_max
            row_total[head] = row_total[head] * rescale + jnp.sum(
                weights, axis=0, keepdims=True
            )
            weighted[head] = weighted[head] * rescale + mix_values(piece(1, head), weights)

    def finish():
        for head in range(kv_count):
            result = (weighted[head] / row_total[head]).T
            for member in range(group):
                attended[:, lanes_of(head * group + member)] = result[
                    member * span : (member + 1) * span
                ].astype(jnp.bfloat16)

    def spread_products(kind):
        def body(step, carry):
            if kind == 0:
                load(step).wait()
            outgoing[kind, step - 1] = jnp.dot(
                attended[...], weight_blocks[step], preferred_element_type=jnp.float32
            ).astype(jnp.bfloat16)
            mix(kind, step).start()
            return carry

        lax.fori_loop(1, parts, body, 0)
        if kind == 0:
            load(0).wait()
        return jnp.dot(attended[...], weight_blocks[0], preferred_element_type=jnp.float32)

    def collect(kind, total):
        for step in range(1, parts):
            mix(kind, step).wait_recv()
            total = total + incoming[kind, step - 1].astype(jnp.float32)
        return total.astype(jnp.bfloat16)

    staying_blocks = run // BLOCK

    def absorb_staying(s, block):
        inner = pl.multiple_of(block * BLOCK, BLOCK)
        at = pl.ds(inner, BLOCK)

        def piece(half, head):
            return lax.select(
                leaving == 0,
                both[s, 1, half, at, lanes_of(head)],
                both[s, 0, half, at, lanes_of(head)],
            )

        absorb(s * run + inner, plan[1], piece)

    for slot in range(slots):
        codes = [plan[4 + link * most + slot] for link in range(2)]

        def step_of(s, carry):
            if slot == 0:
                share(s).wait_recv()
            else:
                for link in range(2):
                    send(link, slot - 1, s).wait_recv()

            def write(link, block, value):
                at = pl.ds(pl.multiple_of(block * BLOCK_ROWS, BLOCK_ROWS), BLOCK_ROWS)
                stage[link, slot, s, at] = value

            pick(s, slot, codes, write)
            for link in range(2):
                send(link, slot, s).start()
            if 1 <= slot <= staying_blocks:
                absorb_staying(s, slot - 1)
            return carry

        lax.fori_loop(0, STREAMS, step_of, 0)
        if slot == 0:
            fresh(1 - leaving)
        if slot == staying_blocks:
            finish()
            own_total = spread_products(0)
            mixed[0] = own_total.astype(jnp.bfloat16)
            fresh(leaving)

    def last_step(s, carry):
        @pl.when(s < STREAMS)
        def _():
            for link in range(2):
                send(link, slots - 1, s).wait_recv()
            for k in range(QUARTERS):
                base = 4 + 2 * most + k
                codes = [plan[base + QUARTERS * core], plan[base + QUARTERS * (1 - core)]]

                def write(index, block, value):
                    at = pl.ds(
                        pl.multiple_of(k * rows + block * BLOCK_ROWS, BLOCK_ROWS), BLOCK_ROWS
                    )
                    if index == 0:
                        final[s, core, at] = value
                    else:
                        hand[s, at] = value

                pick(s, slots, codes, write)
            deliver(s).start()

        @pl.when(s > 0)
        def _():
            before = s - 1
            deliver(before).wait_recv()
            for half in range(2):
                settle(before, half).start()

            def body(block, carry):
                inner = pl.multiple_of(block * BLOCK, BLOCK)
                at = pl.ds(inner, BLOCK)
                absorb(
                    before * run + inner,
                    plan[2],
                    lambda half, head: final[before, half, at, lanes_of(head)],
                )
                return carry

            lax.fori_loop(0, staying_blocks, body, 0)

        return carry

    lax.fori_loop(0, STREAMS + 1, last_step, 0)
    finish()
    arrived_total = spread_products(1)
    staying_mixed = collect(0, mixed[0].astype(jnp.float32))
    arrived_mixed = collect(1, arrived_total)
    mixed[0] = lax.select(leaving == 0, arrived_mixed, staying_mixed)
    mixed[1] = lax.select(leaving == 0, staying_mixed, arrived_mixed)
    for kind in range(2):
        for step in range(1, parts):
            mix(kind, step).wait_send()

    def drain(s, carry):
        share(s).wait_send()
        for slot in range(slots):
            for link in range(2):
                send(link, slot, s).wait_send()
        for half in range(2):
            settle(s, half).wait()
        deliver(s).wait_send()
        return carry

    lax.fori_loop(0, STREAMS, drain, 0)


def route(plan, queries, keys_new, values_new, caches, out_weight, slots, most, identity):
    parts = lax.axis_size("tp")
    slot_count, span, features = queries.shape
    depth = out_weight.shape[0]
    columns = out_weight.shape[1] // parts
    halves, cache_rows, width = caches.shape[1:]
    run = cache_rows // STREAMS
    rows = run // QUARTERS
    kv_count = width // HEAD
    grouped = span * features // width
    anywhere = pl.BlockSpec(memory_space=pl.ANY)
    vmem = pl.BlockSpec(memory_space=pltpu.VMEM)
    kind = jnp.bfloat16
    dma = pltpu.SemaphoreType.DMA
    scratch = [
        pltpu.VMEM((STREAMS, slot_count, halves, run, width), kind),
        pltpu.VMEM((STREAMS, 2 * QUARTERS, rows, width), kind),
        pltpu.VMEM((STREAMS, QUARTERS, rows, width), kind),
        pltpu.VMEM((2, slots, STREAMS, rows, width), kind),
        pltpu.VMEM((2, slots, STREAMS, rows, width), kind),
        pltpu.VMEM((STREAMS, halves, run, width), kind),
        pltpu.VMEM((STREAMS, run, width), kind),
        pltpu.VMEM((kv_count, HEAD, grouped), kind),
        pltpu.VMEM((kv_count, 1, grouped), jnp.float32),
        pltpu.VMEM((kv_count, 1, grouped), jnp.float32),
        pltpu.VMEM((kv_count, HEAD, grouped), jnp.float32),
        pltpu.VMEM((span, features), kind),
        pltpu.VMEM((parts, depth, columns), kind),
        pltpu.VMEM((2, parts - 1, span, columns), kind),
        pltpu.VMEM((2, parts - 1, span, columns), kind),
        dma((STREAMS,)),
        dma((STREAMS,)),
        dma((STREAMS,)),
        dma((2, slots, STREAMS)),
        dma((2, slots, STREAMS)),
        dma((STREAMS, halves)),
        dma((STREAMS,)),
        dma((STREAMS,)),
        dma((parts,)),
        dma((2, parts - 1)),
        dma((2, parts - 1)),
    ]
    return pl.pallas_call(
        functools.partial(route_kernel, slots=slots, most=most),
        out_shape=(
            jax.ShapeDtypeStruct((1, halves, cache_rows, width), kind),
            jax.ShapeDtypeStruct((slot_count, span, columns), kind),
        ),
        in_specs=[pl.BlockSpec(memory_space=pltpu.SMEM), vmem, vmem, vmem, anywhere, anywhere],
        out_specs=(anywhere, vmem),
        scratch_shapes=scratch,
        compiler_params=pltpu.CompilerParams(
            collective_id=identity, has_side_effects=True, vmem_limit_bytes=60 * 1024 * 1024
        ),
        name=f"route{slots}",
    )(plan, queries, keys_new, values_new, caches, out_weight)


def hold_kernel(plan, caches, arrived, held, buffer, in_sem, out_sem):
    leaving = plan[0]
    staying = 1 - leaving
    pieces, halves = in_sem.shape[1:]
    size = buffer.shape[2] // pieces

    def fetch(kind, piece, half):
        at = pl.ds(piece * size, size)
        source = caches.at[staying, half, at] if kind == 0 else arrived.at[0, half, at]
        return pltpu.make_async_copy(
            source, buffer.at[kind, half, at], in_sem.at[kind, piece, half]
        )

    def put(kind, piece, half):
        at = pl.ds(piece * size, size)
        target = held.at[staying if kind == 0 else leaving, half, at]
        return pltpu.make_async_copy(
            buffer.at[kind, half, at], target, out_sem.at[kind, piece, half]
        )

    every = list(itertools.product(range(2), range(pieces), range(halves)))
    for index in every:
        fetch(*index).start()
    for index in every:
        fetch(*index).wait()
        put(*index).start()
    for index in every:
        put(*index).wait()


def hold(plan, caches, arrived):
    anywhere = pl.BlockSpec(memory_space=pl.ANY)
    halves = caches.shape[1]
    return pl.pallas_call(
        hold_kernel,
        out_shape=jax.ShapeDtypeStruct(caches.shape, caches.dtype),
        in_specs=[pl.BlockSpec(memory_space=pltpu.SMEM), anywhere, anywhere],
        out_specs=anywhere,
        scratch_shapes=[
            pltpu.VMEM(caches.shape, caches.dtype),
            pltpu.SemaphoreType.DMA((2, 4, halves)),
            pltpu.SemaphoreType.DMA((2, 4, halves)),
        ],
        name="hold",
    )(plan, caches, arrived)


def migrate(queries, keys_new, values_new, caches, lengths, moving, destination, out_weight):
    slot_count = caches.shape[0]
    span = queries.shape[0] // slot_count
    counts = (5, 6, 8)
    plan = make_plan(lengths, moving, destination, counts)

    def by_slot(array):
        return array.reshape(slot_count, span, array.shape[1])

    arrived, mixed = lax.switch(
        plan[3],
        [
            functools.partial(route, slots=slots, most=counts[-1], identity=2 + index)
            for index, slots in enumerate(counts)
        ],
        plan,
        by_slot(queries),
        by_slot(keys_new),
        by_slot(values_new),
        caches,
        out_weight,
    )
    held = hold(plan, caches, arrived)
    return mixed.reshape(slot_count * span, mixed.shape[2]), held


def on_device(queries, keys_new, values_new, caches, lengths, moving, destination, out_weight):
    replicas = lax.axis_size("rep")
    if replicas == 8:
        return migrate(
            queries, keys_new, values_new, caches, lengths, moving, destination, out_weight
        )
    own_index = lax.axis_index("rep")
    slot_count, _, cache_rows, width = caches.shape
    span = queries.shape[0] // slot_count
    kv_count = width // HEAD
    group = queries.shape[1] // width
    leaving_slot = moving[own_index]
    staying_slot = 1 - leaving_slot
    every = jnp.arange(replicas, dtype=jnp.int32)
    source_of = jnp.sum(
        jnp.where(destination[None, :] == every[:, None], every[None, :], 0), axis=1
    )
    anchor = source_of[own_index]
    incoming_length = lengths[anchor, moving[anchor]]
    staying_length = lengths[own_index, staying_slot]
    query_t = (
        queries.reshape(slot_count, span, kv_count, group, HEAD)
        .transpose(0, 2, 4, 3, 1)
        .reshape(slot_count, kv_count, HEAD, group * span)
    )
    keys_by_slot = keys_new.reshape(slot_count, span, width)
    values_by_slot = values_new.reshape(slot_count, span, width)

    def pick(array, slot):
        return lax.dynamic_index_in_dim(array, slot, 0, keepdims=False)

    held, staying_attended = attend_slot(
        jnp.stack([staying_slot, staying_slot, staying_length]),
        caches,
        pick(query_t, staying_slot),
        pick(keys_by_slot, staying_slot),
        pick(values_by_slot, staying_slot),
        None,
        caches.shape,
    )
    leaving = lax.dynamic_index_in_dim(caches, leaving_slot, 0, keepdims=False)
    piece_rows = 2 * cache_rows // replicas
    pieces = leaving.reshape(replicas, piece_rows, width)
    spread = lax.all_to_all(pieces, "rep", split_axis=0, concat_axis=0, tiled=True)
    ordered = jnp.take(spread, source_of, axis=0, mode="clip")
    arrived = lax.all_to_all(ordered, "rep", split_axis=0, concat_axis=0, tiled=True)
    arrived = arrived.reshape(1, 2, cache_rows, width)
    staying_mixed = project(staying_attended, out_weight, 0)
    held, arrived_attended = attend_slot(
        jnp.stack([jnp.zeros_like(leaving_slot), leaving_slot, incoming_length]),
        arrived,
        pick(query_t, leaving_slot),
        pick(keys_by_slot, leaving_slot),
        pick(values_by_slot, leaving_slot),
        held,
        caches.shape,
    )
    arrived_mixed = project(arrived_attended, out_weight, 1)
    mixed = jnp.where(
        leaving_slot == 0,
        jnp.concatenate([arrived_mixed, staying_mixed], axis=0),
        jnp.concatenate([staying_mixed, arrived_mixed], axis=0),
    )
    return (mixed, held)


def solution(mesh):
    in_specs = (
        P("rep", "tp"),
        P("rep", "tp"),
        P("rep", "tp"),
        P("rep", None, None, "tp"),
        P(),
        P(),
        P(),
        P("tp", None),
    )
    out_specs = (P("rep", "tp"), P("rep", None, None, "tp"))
    return jax.shard_map(
        on_device, mesh=mesh, in_specs=in_specs, out_specs=out_specs, check_vma=False
    )
```

```python
import functools
import itertools
import random

import jax
import jax.numpy as jnp
import numpy as np
from jax import lax
from jax.experimental import pallas as pl
from jax.experimental.pallas import tpu as pltpu
from jax.sharding import PartitionSpec as P

HEAD = 128
BLOCK = 512
LOG2E = 1.4426950408889634
masked_score = -1e30
BLOCK_ROWS = 64


def slot_kernel(
    scalars, source, query_t, keys_fresh, values_fresh, *rest, aliased, kv_count, group
):
    if aliased:
        rest = rest[1:]
    held, attended, cache, row_max, row_total, weighted, in_sem, out_sem = rest
    taken, target, length = scalars[0], scalars[1], scalars[2]
    rows = cache.shape[1]
    blocks = rows // BLOCK
    span = keys_fresh.shape[0]
    factor = HEAD ** (-0.5) * LOG2E

    def fetch(block, part):
        at = pl.ds(pl.multiple_of(block * BLOCK, BLOCK), BLOCK)
        return pltpu.make_async_copy(
            source.at[taken, part, at], cache.at[part, at], in_sem.at[block, part]
        )

    def put(block, part):
        at = pl.ds(pl.multiple_of(block * BLOCK, BLOCK), BLOCK)
        return pltpu.make_async_copy(
            cache.at[part, at], held.at[target, part, at], out_sem.at[block, part]
        )

    for block in range(blocks):
        for part in range(2):
            fetch(block, part).start()

    def scores_of(head, keys):
        return lax.dot_general(
            keys,
            query_t[head],
            (((1,), (0,)), ((), ())),
            preferred_element_type=jnp.float32,
        )

    def mix(values, weights):
        return lax.dot_general(
            values,
            weights.astype(jnp.bfloat16),
            (((0,), (0,)), ((), ())),
            preferred_element_type=jnp.float32,
        )

    key_at = lax.broadcasted_iota(jnp.int32, (span, group * span), 0)
    token_at = lax.broadcasted_iota(jnp.int32, (span, group * span), 1) % span
    for head in range(kv_count):
        lanes = slice(head * HEAD, (head + 1) * HEAD)
        scores = jnp.where(
            key_at <= token_at, scores_of(head, keys_fresh[:, lanes]), masked_score
        )
        new_max = jnp.max(scores, axis=0, keepdims=True)
        weights = jnp.exp2((scores - new_max) * factor)
        row_max[head] = new_max
        row_total[head] = jnp.sum(weights, axis=0, keepdims=True)
        weighted[head] = mix(values_fresh[:, lanes], weights)

    def absorb(block, masked):
        start = pl.multiple_of(block * BLOCK, BLOCK)
        at = pl.ds(start, BLOCK)
        for head in range(kv_count):
            lanes = slice(head * HEAD, (head + 1) * HEAD)
            scores = scores_of(head, cache[0, at, lanes])
            if masked:
                position = start + lax.broadcasted_iota(jnp.int32, scores.shape, 0)
                scores = jnp.where(position < length, scores, masked_score)
            old_max = row_max[head]
            new_max = jnp.maximum(old_max, jnp.max(scores, axis=0, keepdims=True))
            rescale = jnp.exp2((old_max - new_max) * factor)
            weights = jnp.exp2((scores - new_max) * factor)
            row_max[head] = new_max
            row_total[head] = row_total[head] * rescale + jnp.sum(
                weights, axis=0, keepdims=True
            )
            weighted[head] = weighted[head] * rescale + mix(cache[1, at, lanes], weights)

    def step(block, carry):
        for part in range(2):
            fetch(block, part).wait()
            put(block, part).start()
        start = block * BLOCK

        @pl.when(start + BLOCK <= length)
        def _():
            absorb(block, False)

        @pl.when((start < length) & (length < start + BLOCK))
        def _():
            absorb(block, True)

        return carry

    lax.fori_loop(0, blocks, step, 0)
    for head in range(kv_count):
        result = (weighted[head] / row_total[head]).T
        for member in range(group):
            lanes = slice((head * group + member) * HEAD, (head * group + member + 1) * HEAD)
            attended[:, lanes] = result[member * span : (member + 1) * span].astype(
                jnp.bfloat16
            )
    for block in range(blocks):
        for part in range(2):
            put(block, part).wait()


def attend_slot(scalars, source, query_t, keys_fresh, values_fresh, held, held_shape):
    kv_count, _, columns = query_t.shape
    span = keys_fresh.shape[0]
    group = columns // span
    rows, width = source.shape[2:]
    aliased = held is not None
    anywhere = pl.BlockSpec(memory_space=pl.ANY)
    vmem = pl.BlockSpec(memory_space=pltpu.VMEM)
    operands = [scalars, source, query_t, keys_fresh, values_fresh]
    in_specs = [pl.BlockSpec(memory_space=pltpu.SMEM), anywhere, vmem, vmem, vmem]
    if aliased:
        operands.append(held)
        in_specs.append(anywhere)
    blocks = rows // BLOCK
    return pl.pallas_call(
        functools.partial(slot_kernel, aliased=aliased, kv_count=kv_count, group=group),
        out_shape=(
            jax.ShapeDtypeStruct(held_shape, jnp.bfloat16),
            jax.ShapeDtypeStruct((span, kv_count * group * HEAD), jnp.bfloat16),
        ),
        in_specs=in_specs,
        out_specs=(anywhere, vmem),
        scratch_shapes=[
            pltpu.VMEM((2, rows, width), jnp.bfloat16),
            pltpu.VMEM((kv_count, 1, columns), jnp.float32),
            pltpu.VMEM((kv_count, 1, columns), jnp.float32),
            pltpu.VMEM((kv_count, HEAD, columns), jnp.float32),
            pltpu.SemaphoreType.DMA((blocks, 2)),
            pltpu.SemaphoreType.DMA((blocks, 2)),
        ],
        input_output_aliases={5: 0} if aliased else {},
        compiler_params=pltpu.CompilerParams(vmem_limit_bytes=60 * 1024 * 1024),
        cost_estimate=pl.CostEstimate(
            flops=4 * kv_count * columns * (rows + span) * HEAD,
            bytes_accessed=8 * rows * width,
            transcendentals=kv_count * columns * (rows + span),
        ),
    )(*operands)


def project_kernel(
    attended, weight, out, weight_blocks, outgoing, incoming, weight_sem, send_sem, recv_sem
):
    parts = weight_blocks.shape[0]
    own = lax.axis_index("tp")
    columns = out.shape[1]

    def load(step):
        part = lax.rem(own + step, parts)
        at = pl.ds(pl.multiple_of(part * columns, columns), columns)
        return pltpu.make_async_copy(
            weight.at[:, at], weight_blocks.at[step], weight_sem.at[step]
        )

    order = list(range(1, parts)) + [0]
    for step in order:
        load(step).start()
    barrier = pltpu.get_barrier_semaphore()
    for step in range(1, parts):
        pl.semaphore_signal(
            barrier,
            inc=1,
            device_id={"tp": lax.rem(own + step, parts)},
            device_id_type=pl.DeviceIdType.MESH,
        )

    def product(step):
        load(step).wait()
        return jnp.dot(
            attended[...], weight_blocks[step], preferred_element_type=jnp.float32
        )

    copies = []
    for step in range(1, parts):
        outgoing[step - 1] = product(step).astype(jnp.bfloat16)
        if step == 1:
            pl.semaphore_wait(barrier, parts - 1)
        copy = pltpu.make_async_remote_copy(
            src_ref=outgoing.at[step - 1],
            dst_ref=incoming.at[step - 1],
            send_sem=send_sem.at[step - 1],
            recv_sem=recv_sem.at[step - 1],
            device_id={"tp": lax.rem(own + step, parts)},
            device_id_type=pl.DeviceIdType.MESH,
        )
        copy.start()
        copies.append(copy)
    total = product(0)
    for step, copy in enumerate(copies):
        copy.wait_recv()
        total = total + incoming[step].astype(jnp.float32)
    out[...] = total.astype(jnp.bfloat16)
    for copy in copies:
        copy.wait_send()


def project(attended, out_weight, identity):
    parts = lax.axis_size("tp")
    rows, depth = attended.shape
    columns = out_weight.shape[1] // parts
    vmem = pl.BlockSpec(memory_space=pltpu.VMEM)
    return pl.pallas_call(
        project_kernel,
        out_shape=jax.ShapeDtypeStruct((rows, columns), jnp.bfloat16),
        in_specs=[vmem, pl.BlockSpec(memory_space=pl.ANY)],
        out_specs=vmem,
        scratch_shapes=[
            pltpu.VMEM((parts, depth, columns), jnp.bfloat16),
            pltpu.VMEM((parts - 1, rows, columns), jnp.bfloat16),
            pltpu.VMEM((parts - 1, rows, columns), jnp.bfloat16),
            pltpu.SemaphoreType.DMA((parts,)),
            pltpu.SemaphoreType.DMA((parts - 1,)),
            pltpu.SemaphoreType.DMA((parts - 1,)),
        ],
        compiler_params=pltpu.CompilerParams(
            collective_id=identity, has_side_effects=True, vmem_limit_bytes=60 * 1024 * 1024
        ),
        cost_estimate=pl.CostEstimate(
            flops=2 * rows * depth * columns * parts,
            bytes_accessed=2 * depth * columns * parts,
            transcendentals=0,
        ),
        name=f"project{identity}",
    )(attended, out_weight)


QUARTERS = 4
STREAMS = 4


def cut_bound(held_at):
    chips = range(4)
    loads = []
    for bit in (1, 2):
        for side in (0, bit):
            loads.append(
                sum(
                    held_at[c][d]
                    for c in chips
                    for d in chips
                    if c & bit == side and d & bit != side
                )
            )
    for c in chips:
        loads.append(sum(held_at[c][d] for d in chips if d != c))
        loads.append(sum(held_at[d][c] for d in chips if d != c))
    return max(-(-load // 2) for load in loads)


def left_hops(held_at):
    return sum(
        held_at[c][d] * (((c ^ d) & 1) + ((c ^ d) >> 1)) for c in range(4) for d in range(4)
    )


def try_moves(held_at, slots, rng, noise):
    held_at = [row[:] for row in held_at]
    moves = []
    for slot in range(slots):
        left = slots - slot
        hops = left_hops(held_at)
        if hops == 0:
            moves.append({})
            continue
        if hops > 8 * left or cut_bound(held_at) > left:
            return None
        free = [row[:] for row in held_at]
        chosen = {}
        links = [(c, link) for c in range(4) for link in (1, 2)]
        rng.shuffle(links)
        for c, link in links:
            best = None
            for d in range(4):
                if free[c][d] <= 0 or c == d:
                    continue
                if (c ^ d) == 3:
                    value = 2.0 + noise * rng.random()
                elif (c ^ d) & link:
                    value = 1.5 + 0.1 * free[c][d] + noise * rng.random()
                elif left >= 3 and free[c][d] > left - 1:
                    value = 0.5 + 1.5 * noise * rng.random()
                else:
                    continue
                if best is None or value > best[0]:
                    best = (value, d)
            if best:
                chosen[c, link] = best[1]
                free[c][best[1]] -= 1
        for (c, link), d in chosen.items():
            held_at[c][d] -= 1
            held_at[c ^ link][d] += 1
        moves.append(chosen)
    return moves if left_hops(held_at) == 0 else None


def find_moves(demand, rng, most):
    held_at = [[0] * 4 for _ in range(4)]
    for c in range(4):
        for d in demand[c]:
            held_at[c][d] += QUARTERS
    least = max(cut_bound(held_at), -(-left_hops(held_at) // 8))
    for slots in range(least, most + 1):
        for attempt in range(400):
            noise = 0.0 if attempt == 0 else (0.5 if attempt % 2 else 1.5)
            moves = try_moves(held_at, slots, rng, noise)
            if moves is not None:
                return slots, moves
    raise ValueError("no route")


def codes_of(demand, moves, most):
    ready = [[[] for _ in range(4)] for _ in range(4)]
    arriving = []
    for c in range(4):
        for place, d in enumerate(demand[c]):
            for k in range(QUARTERS):
                ready[c][d].append((place * QUARTERS + k, (c, place, k)))
    send = [[[0] * most for _ in range(2)] for _ in range(4)]
    for slot, chosen in enumerate(moves):
        arriving = []
        for (c, link), d in sorted(chosen.items()):
            code, chunk = ready[c][d].pop(0)
            send[c][link - 1][slot] = code
            arriving.append((c ^ link, d, 2 * QUARTERS + 2 * slot + link - 1, chunk))
        for c, d, code, chunk in arriving:
            ready[c][d].append((code, chunk))
    table = []
    for c in range(4):
        here = {chunk: code for code, chunk in ready[c][c]}
        items = sorted({chunk[:2] for chunk in here})
        finals = [here[item + (k,)] for item in items for k in range(QUARTERS)]
        table.append(send[c][0] + send[c][1] + finals)
    return table


@functools.lru_cache
def routes(most):
    pairs = [(a, b) for a in range(4) for b in range(a, 4)]
    rng = random.Random(1)
    place = np.zeros((len(pairs) ** 4,), np.int32)
    rows, slots = [], []
    for index, demand in enumerate(itertools.product(pairs, repeat=4)):
        flat = [d for pair in demand for d in pair]
        if any(flat.count(d) != 2 for d in range(4)):
            continue
        place[index] = len(rows)
        count, moves = find_moves(demand, rng, most)
        rows.append(codes_of(demand, moves, most))
        slots.append(count)
    return place, np.array(rows, np.int32), np.array(slots, np.int32)


def plan_kernel(
    lengths,
    moving,
    destination,
    place,
    rows,
    caches,
    plan,
    branch,
    held,
    found,
    line,
    buffer,
    sem,
    in_sem,
    out_sem,
    *,
    most,
):
    replicas = destination.shape[0]
    staying = 1 - moving[lax.axis_index("rep")]
    fetch_piece, put_piece, every = piece_copies(
        caches, staying, held, staying, buffer, in_sem, out_sem
    )
    for index in every:
        fetch_piece(*index).start()
    own = lax.axis_index("rep")
    chip = own // 2
    key = jnp.int32(0)
    swap = jnp.int32(0)
    for c in range(replicas // 2):
        first, second = destination[2 * c] // 2, destination[2 * c + 1] // 2
        low, high = jnp.minimum(first, second), jnp.maximum(first, second)
        key = key * 10 + low * (7 - low) // 2 + high
        swap = jnp.where(c == chip, (first > second).astype(jnp.int32), swap)
    seek = pltpu.make_async_copy(place.at[key // 128], found, sem)
    seek.start()
    anchor = jnp.int32(0)
    senders = [jnp.int32(0), jnp.int32(0)]
    for r in range(replicas):
        goal = destination[r]
        anchor = jnp.where(goal == own, r, anchor)
        senders = [
            jnp.where(goal == 2 * chip + index, r, sender)
            for index, sender in enumerate(senders)
        ]
    crossed = (senders[0] > senders[1]).astype(jnp.int32)
    leaving = moving[own]
    plan[0] = leaving
    at_row = lax.broadcasted_iota(jnp.int32, lengths.shape, 0)
    at_slot = lax.broadcasted_iota(jnp.int32, lengths.shape, 1)
    length_of = lengths[...].astype(jnp.float32)

    def look_up(row, slot):
        here = (at_row == row) & (at_slot == slot)
        return jnp.sum(jnp.where(here, length_of, 0.0)).astype(jnp.int32)

    plan[1] = look_up(own, 1 - leaving)
    plan[2] = look_up(anchor, moving[anchor])
    seek.wait()
    fetch = pltpu.make_async_copy(rows.at[found[0, key % 128]], line, sem)
    fetch.start()
    fetch.wait()
    branch[0] = line[0, line.shape[1] - 1]
    size = 2 * most + 2 * QUARTERS
    for index in range(size):
        at = index
        if index >= 2 * most:
            final = index - 2 * most
            at = 2 * most + (final + QUARTERS * crossed) % (2 * QUARTERS)
        code = line[0, chip * size + at]
        turned = (code + QUARTERS * swap) % (2 * QUARTERS)
        plan[4 + index] = jnp.where(code < 2 * QUARTERS, turned, code)
    for index in every:
        fetch_piece(*index).wait()
        put_piece(*index).start()
    for index in every:
        put_piece(*index).wait()


def piece_copies(source, source_slot, held, target_slot, buffer, in_sem, out_sem):
    pieces, halves = in_sem.shape
    size = buffer.shape[1] // pieces

    def fetch(piece, half):
        at = pl.ds(piece * size, size)
        return pltpu.make_async_copy(
            source.at[source_slot, half, at], buffer.at[half, at], in_sem.at[piece, half]
        )

    def put(piece, half):
        at = pl.ds(piece * size, size)
        return pltpu.make_async_copy(
            buffer.at[half, at], held.at[target_slot, half, at], out_sem.at[piece, half]
        )

    return fetch, put, list(itertools.product(range(pieces), range(halves)))


def make_plan(lengths, moving, destination, caches, counts):
    most = counts[-1]
    place, rows, slots = routes(most)
    lines = -(-place.size // 128)
    places = np.zeros((lines * 128,), np.int32)
    places[: place.size] = place
    table = np.zeros((rows.shape[0], 1, 128), np.int32)
    table[:, 0, : rows[0].size] = rows.reshape(rows.shape[0], -1)
    table[:, 0, 127] = np.sum(slots[:, None] > np.array(counts[:-1]), axis=1)
    anywhere = pl.BlockSpec(memory_space=pl.ANY)
    smem = pl.BlockSpec(memory_space=pltpu.SMEM)
    return pl.pallas_call(
        functools.partial(plan_kernel, most=most),
        out_shape=(
            jax.ShapeDtypeStruct((4 + 2 * most + 2 * QUARTERS,), jnp.int32),
            jax.ShapeDtypeStruct((1,), jnp.int32),
            jax.ShapeDtypeStruct(caches.shape, caches.dtype),
        ),
        in_specs=[
            pl.BlockSpec(memory_space=pltpu.VMEM),
            smem,
            smem,
            anywhere,
            anywhere,
            anywhere,
        ],
        out_specs=(smem, smem, anywhere),
        scratch_shapes=[
            pltpu.SMEM((1, 128), jnp.int32),
            pltpu.SMEM((1, 128), jnp.int32),
            pltpu.VMEM(caches.shape[1:], caches.dtype),
            pltpu.SemaphoreType.DMA,
            pltpu.SemaphoreType.DMA((4, caches.shape[1])),
            pltpu.SemaphoreType.DMA((4, caches.shape[1])),
        ],
        name="plan",
    )(
        lengths,
        moving,
        destination,
        jnp.asarray(places.reshape(lines, 1, 128)),
        jnp.asarray(table),
        caches,
    )


def route_kernel(
    plan,
    queries_from,
    keys_from,
    values_from,
    caches,
    weight,
    arrived,
    mixed,
    queries,
    keys_new,
    values_new,
    both,
    local,
    give,
    arr,
    stage,
    final,
    hand,
    query_t,
    row_max,
    row_total,
    weighted,
    attended,
    weight_blocks,
    outgoing,
    incoming,
    totals,
    fresh_sem,
    in_sem,
    give_sem,
    gave_sem,
    send_sem,
    recv_sem,
    keep_sem,
    hand_sem,
    got_sem,
    weight_sem,
    out_sem,
    mix_sem,
    *,
    slots,
    most,
):
    own = lax.axis_index("rep")
    part = lax.axis_index("tp")
    parts = weight_blocks.shape[0]
    core = own % 2
    partner = own + 1 - 2 * core
    across = (own + 2 - 4 * ((own // 2) % 2), own + 4 - 8 * (own // 4))
    rows = stage.shape[3]
    span, columns = mixed.shape[1:]
    kv_count = query_t.shape[0]
    group = query_t.shape[2] // span
    run = QUARTERS * rows
    factor = HEAD ** (-0.5) * LOG2E
    leaving = plan[0]

    def fetch(s):
        return pltpu.make_async_copy(
            caches.at[:, :, pl.ds(s * run, run)], both.at[s], in_sem.at[s]
        )

    def load(step):
        at = pl.ds(pl.multiple_of(lax.rem(part + step, parts) * columns, columns), columns)
        return pltpu.make_async_copy(
            weight.at[:, at], weight_blocks.at[step], weight_sem.at[step]
        )

    fresh_copies = [
        pltpu.make_async_copy(source, into, fresh_sem.at[index])
        for index, (source, into) in enumerate(
            ((queries_from, queries), (keys_from, keys_new), (values_from, values_new))
        )
    ]
    for s in range(STREAMS):
        fetch(s).start()
    barrier = pltpu.get_barrier_semaphore()
    peers = [{"rep": partner}] + [{"rep": peer} for peer in across]
    peers += [{"tp": lax.rem(part + step, parts)} for step in range(1, parts)]
    for peer in peers:
        pl.semaphore_signal(
            barrier, inc=1, device_id=peer, device_id_type=pl.DeviceIdType.MESH
        )

    def remote(src, dst, send, recv, peer):
        return pltpu.make_async_remote_copy(
            src_ref=src,
            dst_ref=dst,
            send_sem=send,
            recv_sem=recv,
            device_id=peer,
            device_id_type=pl.DeviceIdType.MESH,
        )

    def share(s):
        return remote(
            give.at[s],
            local.at[s, pl.ds(core * QUARTERS, QUARTERS)],
            give_sem.at[s],
            gave_sem.at[s],
            {"rep": partner},
        )

    def send(link, slot, s):
        return remote(
            stage.at[link, slot, s],
            arr.at[link, slot, s],
            send_sem.at[link, slot, s],
            recv_sem.at[link, slot, s],
            {"rep": across[link]},
        )

    def settle(s, half):
        return pltpu.make_async_copy(
            final.at[s, half],
            arrived.at[0, half, pl.ds(s * run, run)],
            keep_sem.at[s, half],
        )

    def deliver(s):
        return remote(
            hand.at[s],
            final.at[s, core],
            hand_sem.at[s],
            got_sem.at[s],
            {"rep": partner},
        )

    def mix(kind, index, place, target):
        return remote(
            outgoing.at[kind, index],
            incoming.at[kind, place],
            out_sem.at[kind, index],
            mix_sem.at[kind, place],
            {"tp": target},
        )

    def pick(s, upto, codes, write):
        def body(block, carry):
            at = pl.ds(pl.multiple_of(block * BLOCK_ROWS, BLOCK_ROWS), BLOCK_ROWS)
            values = [local[s, 0, at]] * len(codes)
            came = [(home, local[s, home, at]) for home in range(1, 2 * QUARTERS)]
            came += [
                (2 * QUARTERS + 2 * slot + link, arr[link, slot, s, at])
                for slot in range(upto)
                for link in range(2)
            ]
            for here, piece in came:
                values = [
                    lax.select(code == here, piece, value)
                    for code, value in zip(codes, values)
                ]
            for index, value in enumerate(values):
                write(index, block, value)
            return carry

        lax.fori_loop(0, rows // BLOCK_ROWS, body, 0)

    def share_out(s, carry):
        fetch(s).wait()

        def body(block, carry):
            k = block // (rows // BLOCK_ROWS)
            inner = pl.multiple_of(block % (rows // BLOCK_ROWS) * BLOCK_ROWS, BLOCK_ROWS)
            at = pl.ds(pl.multiple_of(block * BLOCK_ROWS, BLOCK_ROWS), BLOCK_ROWS)
            to = pl.ds(inner, BLOCK_ROWS)
            for half, into in ((1 - core, None), (core, core)):
                value = lax.select(
                    leaving == 0, both[s, 0, half, at], both[s, 1, half, at]
                )
                if into is None:
                    give[s, k, to] = value
                else:
                    local[s, core * QUARTERS + k, to] = value
            return carry

        lax.fori_loop(0, run // BLOCK_ROWS, body, 0)

        @pl.when(s == 0)
        def _():
            pl.semaphore_wait(barrier, len(peers))

        share(s).start()

        return carry

    lax.fori_loop(0, STREAMS, share_out, 0)
    for copy in fresh_copies:
        copy.start()
    for step in list(range(1, parts)) + [0]:
        load(step).start()

    def lanes_of(head):
        return slice(head * HEAD, (head + 1) * HEAD)

    def mix_values(values, weights):
        return lax.dot_general(
            values,
            weights.astype(jnp.bfloat16),
            (((0,), (0,)), ((), ())),
            preferred_element_type=jnp.float32,
        )

    def scores_of(head, keys):
        return lax.dot_general(
            keys,
            query_t[head],
            (((1,), (0,)), ((), ())),
            preferred_element_type=jnp.float32,
        )

    def fresh(slot):
        def choose(ref, lanes):
            return lax.select(slot == 0, ref[0, :, lanes], ref[1, :, lanes])

        key_at = lax.broadcasted_iota(jnp.int32, (span, group * span), 0)
        token_at = lax.broadcasted_iota(jnp.int32, (span, group * span), 1) % span
        for head in range(kv_count):
            for member in range(group):
                query_t[head, :, member * span : (member + 1) * span] = choose(
                    queries, lanes_of(head * group + member)
                ).T
            scores = jnp.where(
                key_at <= token_at, scores_of(head, choose(keys_new, lanes_of(head))), masked_score
            )
            new_max = jnp.max(scores, axis=0, keepdims=True)
            weights = jnp.exp2((scores - new_max) * factor)
            row_max[head] = new_max
            row_total[head] = jnp.sum(weights, axis=0, keepdims=True)
            weighted[head] = mix_values(choose(values_new, lanes_of(head)), weights)

    def absorb(start, length, piece):
        for head in range(kv_count):
            scores = scores_of(head, piece(0, head))
            position = start + lax.broadcasted_iota(jnp.int32, scores.shape, 0)
            scores = jnp.where(position < length, scores, masked_score)
            old_max = row_max[head]
            new_max = jnp.maximum(old_max, jnp.max(scores, axis=0, keepdims=True))
            rescale = jnp.exp2((old_max - new_max) * factor)
            weights = jnp.exp2((scores - new_max) * factor)
            row_max[head] = new_max
            row_total[head] = row_total[head] * rescale + jnp.sum(
                weights, axis=0, keepdims=True
            )
            weighted[head] = weighted[head] * rescale + mix_values(piece(1, head), weights)

    def finish():
        for head in range(kv_count):
            result = (weighted[head] / row_total[head]).T
            for member in range(group):
                attended[:, lanes_of(head * group + member)] = result[
                    member * span : (member + 1) * span
                ].astype(jnp.bfloat16)

    relayed = parts == 4
    low = part < parts // 2
    edge = (part == 0) | (part == parts - 1)

    def mirror(place):
        return jnp.where(low, place, parts - 1 - place)

    def product(column):
        step = lax.rem(column - part + parts, parts)
        return jnp.dot(
            attended[...], weight_blocks[step], preferred_element_type=jnp.float32
        )

    def spread_direct(kind):
        def body(index, carry):
            column = lax.rem(part + 1 + index, parts)
            if kind == 0:
                load(lax.rem(index + 1, parts)).wait()
            value = product(column)

            @pl.when(index < parts - 1)
            def _():
                outgoing[kind, index] = value.astype(jnp.bfloat16)
                mix(kind, index, part, column).start()

            @pl.when(index == parts - 1)
            def _():
                totals[kind] = value

            return carry

        lax.fori_loop(0, parts, body, 0)

    def collect_direct(kind):
        for step in range(1, parts):
            place = lax.rem(part + step, parts)
            mix(kind, 0, place, place).wait_recv()
            totals[kind] += incoming[kind, place].astype(jnp.float32)

    def spread_relayed(kind):
        def body(index, carry):
            goal = jnp.where(
                edge,
                jnp.where(index < 2, 3 - index, jnp.where(index == 2, 0, 1)),
                jnp.where(index == 0, 2, jnp.where(index == 1, 0, index * 2 - 3)),
            )
            value = product(mirror(goal))
            slot = jnp.where(index < 2, index, 2)

            @pl.when(index == 2)
            def _():
                totals[kind] = value

            @pl.when((index != 2) & ((index < 3) | edge))
            def _():
                outgoing[kind, slot] = value.astype(jnp.bfloat16)

            @pl.when((index == 3) & jnp.logical_not(edge))
            def _():
                mix(kind, 2, parts, part).wait_recv()
                outgoing[kind, slot] = (
                    value + incoming[kind, parts].astype(jnp.float32)
                ).astype(jnp.bfloat16)

            @pl.when(index != 2)
            def _():
                first = edge & (index == 0)
                mix(
                    kind,
                    slot,
                    jnp.where(first, parts, part),
                    mirror(jnp.where(first, 1, goal)),
                ).start()

            return carry

        lax.fori_loop(0, parts, body, 0)

    def collect_relayed(kind):
        def take(place):
            mix(kind, 0, mirror(place), part).wait_recv()
            totals[kind] += incoming[kind, mirror(place)].astype(jnp.float32)

        @pl.when(edge)
        def _():
            take(1)

        @pl.when(jnp.logical_not(edge))
        def _():
            take(0)
            take(3)

        take(2)

    spread_arrived = spread_relayed if relayed else spread_direct
    collect_arrived = collect_relayed if relayed else collect_direct

    staying_blocks = run // BLOCK

    def absorb_staying(s, block):
        inner = pl.multiple_of(block * BLOCK, BLOCK)
        at = pl.ds(inner, BLOCK)

        def piece(half, head):
            return lax.select(
                leaving == 0,
                both[s, 1, half, at, lanes_of(head)],
                both[s, 0, half, at, lanes_of(head)],
            )

        absorb(s * run + inner, plan[1], piece)

    for slot in range(slots):
        codes = [plan[4 + link * most + slot] for link in range(2)]

        def step_of(s, carry):
            if slot == 0:
                share(s).wait_recv()
            else:
                for link in range(2):
                    send(link, slot - 1, s).wait_recv()

            def write(link, block, value):
                at = pl.ds(pl.multiple_of(block * BLOCK_ROWS, BLOCK_ROWS), BLOCK_ROWS)
                stage[link, slot, s, at] = value

            pick(s, slot, codes, write)
            for link in range(2):
                send(link, slot, s).start()
            if 1 <= slot <= staying_blocks:
                absorb_staying(s, slot - 1)
            return carry

        lax.fori_loop(0, STREAMS, step_of, 0)
        if slot == 0:
            for copy in fresh_copies:
                copy.wait()
            fresh(1 - leaving)
        if slot == staying_blocks:
            finish()
            spread_direct(0)
            fresh(leaving)

    def last_step(s, carry):
        @pl.when(s < STREAMS)
        def _():
            for link in range(2):
                send(link, slots - 1, s).wait_recv()
            for k in range(QUARTERS):
                base = 4 + 2 * most + k
                codes = [plan[base + QUARTERS * core], plan[base + QUARTERS * (1 - core)]]

                def write(index, block, value):
                    at = pl.ds(
                        pl.multiple_of(k * rows + block * BLOCK_ROWS, BLOCK_ROWS), BLOCK_ROWS
                    )
                    if index == 0:
                        final[s, core, at] = value
                    else:
                        hand[s, at] = value

                pick(s, slots, codes, write)
            deliver(s).start()

        @pl.when(s > 0)
        def _():
            before = s - 1
            deliver(before).wait_recv()
            for half in range(2):
                settle(before, half).start()

            def body(block, carry):
                inner = pl.multiple_of(block * BLOCK, BLOCK)
                at = pl.ds(inner, BLOCK)
                absorb(
                    before * run + inner,
                    plan[2],
                    lambda half, head: final[before, half, at, lanes_of(head)],
                )
                return carry

            lax.fori_loop(0, staying_blocks, body, 0)

        return carry

    lax.fori_loop(0, STREAMS + 1, last_step, 0)
    finish()
    spread_arrived(1)
    collect_direct(0)
    staying_mixed = totals[0].astype(jnp.bfloat16)
    collect_arrived(1)
    arrived_mixed = totals[1].astype(jnp.bfloat16)
    mixed[0] = lax.select(leaving == 0, arrived_mixed, staying_mixed)
    mixed[1] = lax.select(leaving == 0, staying_mixed, arrived_mixed)
    for kind in range(2):
        for index in range(parts - 1):
            mix(kind, index, part, lax.rem(part + 1, parts)).wait_send()

    def drain(s, carry):
        share(s).wait_send()
        for slot in range(slots):
            for link in range(2):
                send(link, slot, s).wait_send()
        for half in range(2):
            settle(s, half).wait()
        deliver(s).wait_send()
        return carry

    lax.fori_loop(0, STREAMS, drain, 0)


def route(plan, queries, keys_new, values_new, caches, out_weight, slots, most, identity):
    parts = lax.axis_size("tp")
    slot_count, span, features = queries.shape
    depth = out_weight.shape[0]
    columns = out_weight.shape[1] // parts
    halves, cache_rows, width = caches.shape[1:]
    run = cache_rows // STREAMS
    rows = run // QUARTERS
    kv_count = width // HEAD
    grouped = span * features // width
    anywhere = pl.BlockSpec(memory_space=pl.ANY)
    vmem = pl.BlockSpec(memory_space=pltpu.VMEM)
    kind = jnp.bfloat16
    dma = pltpu.SemaphoreType.DMA
    scratch = [
        pltpu.VMEM(queries.shape, kind),
        pltpu.VMEM(keys_new.shape, kind),
        pltpu.VMEM(values_new.shape, kind),
        pltpu.VMEM((STREAMS, slot_count, halves, run, width), kind),
        pltpu.VMEM((STREAMS, 2 * QUARTERS, rows, width), kind),
        pltpu.VMEM((STREAMS, QUARTERS, rows, width), kind),
        pltpu.VMEM((2, slots, STREAMS, rows, width), kind),
        pltpu.VMEM((2, slots, STREAMS, rows, width), kind),
        pltpu.VMEM((STREAMS, halves, run, width), kind),
        pltpu.VMEM((STREAMS, run, width), kind),
        pltpu.VMEM((kv_count, HEAD, grouped), kind),
        pltpu.VMEM((kv_count, 1, grouped), jnp.float32),
        pltpu.VMEM((kv_count, 1, grouped), jnp.float32),
        pltpu.VMEM((kv_count, HEAD, grouped), jnp.float32),
        pltpu.VMEM((span, features), kind),
        pltpu.VMEM((parts, depth, columns), kind),
        pltpu.VMEM((2, parts - 1, span, columns), kind),
        pltpu.VMEM((2, parts + 1, span, columns), kind),
        pltpu.VMEM((2, span, columns), jnp.float32),
        dma((3,)),
        dma((STREAMS,)),
        dma((STREAMS,)),
        dma((STREAMS,)),
        dma((2, slots, STREAMS)),
        dma((2, slots, STREAMS)),
        dma((STREAMS, halves)),
        dma((STREAMS,)),
        dma((STREAMS,)),
        dma((parts,)),
        dma((2, parts - 1)),
        dma((2, parts + 1)),
    ]
    return pl.pallas_call(
        functools.partial(route_kernel, slots=slots, most=most),
        out_shape=(
            jax.ShapeDtypeStruct((1, halves, cache_rows, width), kind),
            jax.ShapeDtypeStruct((slot_count, span, columns), kind),
        ),
        in_specs=[pl.BlockSpec(memory_space=pltpu.SMEM)] + [anywhere] * 5,
        out_specs=(anywhere, vmem),
        scratch_shapes=scratch,
        compiler_params=pltpu.CompilerParams(
            collective_id=identity, has_side_effects=True, vmem_limit_bytes=60 * 1024 * 1024
        ),
        name=f"route{slots}",
    )(plan, queries, keys_new, values_new, caches, out_weight)


def hold_kernel(plan, arrived, mixed, _, out, held, buffer, in_sem, out_sem):
    leaving = plan[0]
    fetch, put, every = piece_copies(arrived, 0, held, leaving, buffer, in_sem, out_sem)
    for index in every:
        fetch(*index).start()
    out[...] = mixed[...]
    for index in every:
        fetch(*index).wait()
        put(*index).start()
    for index in every:
        put(*index).wait()


def hold(plan, arrived, mixed, held):
    anywhere = pl.BlockSpec(memory_space=pl.ANY)
    vmem = pl.BlockSpec(memory_space=pltpu.VMEM)
    return pl.pallas_call(
        hold_kernel,
        out_shape=(
            jax.ShapeDtypeStruct(mixed.shape, mixed.dtype),
            jax.ShapeDtypeStruct(held.shape, held.dtype),
        ),
        in_specs=[pl.BlockSpec(memory_space=pltpu.SMEM), anywhere, vmem, anywhere],
        out_specs=(vmem, anywhere),
        scratch_shapes=[
            pltpu.VMEM(held.shape[1:], held.dtype),
            pltpu.SemaphoreType.DMA((4, held.shape[1])),
            pltpu.SemaphoreType.DMA((4, held.shape[1])),
        ],
        input_output_aliases={3: 1},
        name="hold",
    )(plan, arrived, mixed, held)


def migrate(queries, keys_new, values_new, caches, lengths, moving, destination, out_weight):
    slot_count = caches.shape[0]
    span = queries.shape[0] // slot_count
    counts = (5, 6, 8)
    plan, branch, held = make_plan(lengths, moving, destination, caches, counts)

    def by_slot(array):
        return array.reshape(slot_count, span, array.shape[1])

    arrived, mixed = lax.switch(
        branch[0],
        [
            functools.partial(route, slots=slots, most=counts[-1], identity=2 + index)
            for index, slots in enumerate(counts)
        ],
        plan,
        by_slot(queries),
        by_slot(keys_new),
        by_slot(values_new),
        caches,
        out_weight,
    )
    mixed, held = hold(plan, arrived, mixed, held)
    return mixed.reshape(slot_count * span, mixed.shape[2]), held


def on_device(queries, keys_new, values_new, caches, lengths, moving, destination, out_weight):
    replicas = lax.axis_size("rep")
    if replicas == 8:
        return migrate(
            queries, keys_new, values_new, caches, lengths, moving, destination, out_weight
        )
    own_index = lax.axis_index("rep")
    slot_count, _, cache_rows, width = caches.shape
    span = queries.shape[0] // slot_count
    kv_count = width // HEAD
    group = queries.shape[1] // width
    leaving_slot = moving[own_index]
    staying_slot = 1 - leaving_slot
    every = jnp.arange(replicas, dtype=jnp.int32)
    source_of = jnp.sum(
        jnp.where(destination[None, :] == every[:, None], every[None, :], 0), axis=1
    )
    anchor = source_of[own_index]
    incoming_length = lengths[anchor, moving[anchor]]
    staying_length = lengths[own_index, staying_slot]
    query_t = (
        queries.reshape(slot_count, span, kv_count, group, HEAD)
        .transpose(0, 2, 4, 3, 1)
        .reshape(slot_count, kv_count, HEAD, group * span)
    )
    keys_by_slot = keys_new.reshape(slot_count, span, width)
    values_by_slot = values_new.reshape(slot_count, span, width)

    def pick(array, slot):
        return lax.dynamic_index_in_dim(array, slot, 0, keepdims=False)

    held, staying_attended = attend_slot(
        jnp.stack([staying_slot, staying_slot, staying_length]),
        caches,
        pick(query_t, staying_slot),
        pick(keys_by_slot, staying_slot),
        pick(values_by_slot, staying_slot),
        None,
        caches.shape,
    )
    leaving = lax.dynamic_index_in_dim(caches, leaving_slot, 0, keepdims=False)
    piece_rows = 2 * cache_rows // replicas
    pieces = leaving.reshape(replicas, piece_rows, width)
    spread = lax.all_to_all(pieces, "rep", split_axis=0, concat_axis=0, tiled=True)
    ordered = jnp.take(spread, source_of, axis=0, mode="clip")
    arrived = lax.all_to_all(ordered, "rep", split_axis=0, concat_axis=0, tiled=True)
    arrived = arrived.reshape(1, 2, cache_rows, width)
    staying_mixed = project(staying_attended, out_weight, 0)
    held, arrived_attended = attend_slot(
        jnp.stack([jnp.zeros_like(leaving_slot), leaving_slot, incoming_length]),
        arrived,
        pick(query_t, leaving_slot),
        pick(keys_by_slot, leaving_slot),
        pick(values_by_slot, leaving_slot),
        held,
        caches.shape,
    )
    arrived_mixed = project(arrived_attended, out_weight, 1)
    mixed = jnp.where(
        leaving_slot == 0,
        jnp.concatenate([arrived_mixed, staying_mixed], axis=0),
        jnp.concatenate([staying_mixed, arrived_mixed], axis=0),
    )
    return (mixed, held)


def solution(mesh):
    in_specs = (
        P("rep", "tp"),
        P("rep", "tp"),
        P("rep", "tp"),
        P("rep", None, None, "tp"),
        P(),
        P(),
        P(),
        P("tp", None),
    )
    out_specs = (P("rep", "tp"), P("rep", None, None, "tp"))
    return jax.shard_map(
        on_device, mesh=mesh, in_specs=in_specs, out_specs=out_specs, check_vma=False
    )
```

```python
import functools
import itertools
import random

import jax
import jax.numpy as jnp
import numpy as np
from jax import lax
from jax.experimental import pallas as pl
from jax.experimental.pallas import tpu as pltpu
from jax.sharding import PartitionSpec as P

HEAD = 128
BLOCK = 512
LOG2E = 1.4426950408889634
masked_score = -1e30
BLOCK_ROWS = 64
LENGTH_STEP = 128


def slot_kernel(
    scalars, source, query_t, keys_fresh, values_fresh, *rest, aliased, kv_count, group
):
    if aliased:
        rest = rest[1:]
    held, attended, cache, row_max, row_total, weighted, in_sem, out_sem = rest
    taken, target, length = scalars[0], scalars[1], scalars[2]
    rows = cache.shape[1]
    blocks = rows // BLOCK
    span = keys_fresh.shape[0]
    factor = HEAD ** (-0.5) * LOG2E

    def fetch(block, part):
        at = pl.ds(pl.multiple_of(block * BLOCK, BLOCK), BLOCK)
        return pltpu.make_async_copy(
            source.at[taken, part, at], cache.at[part, at], in_sem.at[block, part]
        )

    def put(block, part):
        at = pl.ds(pl.multiple_of(block * BLOCK, BLOCK), BLOCK)
        return pltpu.make_async_copy(
            cache.at[part, at], held.at[target, part, at], out_sem.at[block, part]
        )

    for block in range(blocks):
        for part in range(2):
            fetch(block, part).start()

    def scores_of(head, keys):
        return lax.dot_general(
            keys,
            query_t[head],
            (((1,), (0,)), ((), ())),
            preferred_element_type=jnp.float32,
        )

    def mix(values, weights):
        return lax.dot_general(
            values,
            weights.astype(jnp.bfloat16),
            (((0,), (0,)), ((), ())),
            preferred_element_type=jnp.float32,
        )

    key_at = lax.broadcasted_iota(jnp.int32, (span, group * span), 0)
    token_at = lax.broadcasted_iota(jnp.int32, (span, group * span), 1) % span
    for head in range(kv_count):
        lanes = slice(head * HEAD, (head + 1) * HEAD)
        scores = jnp.where(
            key_at <= token_at, scores_of(head, keys_fresh[:, lanes]), masked_score
        )
        new_max = jnp.max(scores, axis=0, keepdims=True)
        weights = jnp.exp2((scores - new_max) * factor)
        row_max[head] = new_max
        row_total[head] = jnp.sum(weights, axis=0, keepdims=True)
        weighted[head] = mix(values_fresh[:, lanes], weights)

    def absorb(block, masked):
        start = pl.multiple_of(block * BLOCK, BLOCK)
        at = pl.ds(start, BLOCK)
        for head in range(kv_count):
            lanes = slice(head * HEAD, (head + 1) * HEAD)
            scores = scores_of(head, cache[0, at, lanes])
            if masked:
                position = start + lax.broadcasted_iota(jnp.int32, scores.shape, 0)
                scores = jnp.where(position < length, scores, masked_score)
            old_max = row_max[head]
            new_max = jnp.maximum(old_max, jnp.max(scores, axis=0, keepdims=True))
            rescale = jnp.exp2((old_max - new_max) * factor)
            weights = jnp.exp2((scores - new_max) * factor)
            row_max[head] = new_max
            row_total[head] = row_total[head] * rescale + jnp.sum(
                weights, axis=0, keepdims=True
            )
            weighted[head] = weighted[head] * rescale + mix(cache[1, at, lanes], weights)

    def step(block, carry):
        for part in range(2):
            fetch(block, part).wait()
            put(block, part).start()
        start = block * BLOCK

        @pl.when(start + BLOCK <= length)
        def _():
            absorb(block, False)

        @pl.when((start < length) & (length < start + BLOCK))
        def _():
            absorb(block, True)

        return carry

    lax.fori_loop(0, blocks, step, 0)
    for head in range(kv_count):
        result = (weighted[head] / row_total[head]).T
        for member in range(group):
            lanes = slice((head * group + member) * HEAD, (head * group + member + 1) * HEAD)
            attended[:, lanes] = result[member * span : (member + 1) * span].astype(
                jnp.bfloat16
            )
    for block in range(blocks):
        for part in range(2):
            put(block, part).wait()


def attend_slot(scalars, source, query_t, keys_fresh, values_fresh, held, held_shape):
    kv_count, _, columns = query_t.shape
    span = keys_fresh.shape[0]
    group = columns // span
    rows, width = source.shape[2:]
    aliased = held is not None
    anywhere = pl.BlockSpec(memory_space=pl.ANY)
    vmem = pl.BlockSpec(memory_space=pltpu.VMEM)
    operands = [scalars, source, query_t, keys_fresh, values_fresh]
    in_specs = [pl.BlockSpec(memory_space=pltpu.SMEM), anywhere, vmem, vmem, vmem]
    if aliased:
        operands.append(held)
        in_specs.append(anywhere)
    blocks = rows // BLOCK
    return pl.pallas_call(
        functools.partial(slot_kernel, aliased=aliased, kv_count=kv_count, group=group),
        out_shape=(
            jax.ShapeDtypeStruct(held_shape, jnp.bfloat16),
            jax.ShapeDtypeStruct((span, kv_count * group * HEAD), jnp.bfloat16),
        ),
        in_specs=in_specs,
        out_specs=(anywhere, vmem),
        scratch_shapes=[
            pltpu.VMEM((2, rows, width), jnp.bfloat16),
            pltpu.VMEM((kv_count, 1, columns), jnp.float32),
            pltpu.VMEM((kv_count, 1, columns), jnp.float32),
            pltpu.VMEM((kv_count, HEAD, columns), jnp.float32),
            pltpu.SemaphoreType.DMA((blocks, 2)),
            pltpu.SemaphoreType.DMA((blocks, 2)),
        ],
        input_output_aliases={5: 0} if aliased else {},
        compiler_params=pltpu.CompilerParams(vmem_limit_bytes=60 * 1024 * 1024),
        cost_estimate=pl.CostEstimate(
            flops=4 * kv_count * columns * (rows + span) * HEAD,
            bytes_accessed=8 * rows * width,
            transcendentals=kv_count * columns * (rows + span),
        ),
    )(*operands)


def project_kernel(
    attended, weight, out, weight_blocks, outgoing, incoming, weight_sem, send_sem, recv_sem
):
    parts = weight_blocks.shape[0]
    own = lax.axis_index("tp")
    columns = out.shape[1]

    def load(step):
        part = lax.rem(own + step, parts)
        at = pl.ds(pl.multiple_of(part * columns, columns), columns)
        return pltpu.make_async_copy(
            weight.at[:, at], weight_blocks.at[step], weight_sem.at[step]
        )

    order = list(range(1, parts)) + [0]
    for step in order:
        load(step).start()
    barrier = pltpu.get_barrier_semaphore()
    for step in range(1, parts):
        pl.semaphore_signal(
            barrier,
            inc=1,
            device_id={"tp": lax.rem(own + step, parts)},
            device_id_type=pl.DeviceIdType.MESH,
        )

    def product(step):
        load(step).wait()
        return jnp.dot(
            attended[...], weight_blocks[step], preferred_element_type=jnp.float32
        )

    copies = []
    for step in range(1, parts):
        outgoing[step - 1] = product(step).astype(jnp.bfloat16)
        if step == 1:
            pl.semaphore_wait(barrier, parts - 1)
        copy = pltpu.make_async_remote_copy(
            src_ref=outgoing.at[step - 1],
            dst_ref=incoming.at[step - 1],
            send_sem=send_sem.at[step - 1],
            recv_sem=recv_sem.at[step - 1],
            device_id={"tp": lax.rem(own + step, parts)},
            device_id_type=pl.DeviceIdType.MESH,
        )
        copy.start()
        copies.append(copy)
    total = product(0)
    for step, copy in enumerate(copies):
        copy.wait_recv()
        total = total + incoming[step].astype(jnp.float32)
    out[...] = total.astype(jnp.bfloat16)
    for copy in copies:
        copy.wait_send()


def project(attended, out_weight, identity):
    parts = lax.axis_size("tp")
    rows, depth = attended.shape
    columns = out_weight.shape[1] // parts
    vmem = pl.BlockSpec(memory_space=pltpu.VMEM)
    return pl.pallas_call(
        project_kernel,
        out_shape=jax.ShapeDtypeStruct((rows, columns), jnp.bfloat16),
        in_specs=[vmem, pl.BlockSpec(memory_space=pl.ANY)],
        out_specs=vmem,
        scratch_shapes=[
            pltpu.VMEM((parts, depth, columns), jnp.bfloat16),
            pltpu.VMEM((parts - 1, rows, columns), jnp.bfloat16),
            pltpu.VMEM((parts - 1, rows, columns), jnp.bfloat16),
            pltpu.SemaphoreType.DMA((parts,)),
            pltpu.SemaphoreType.DMA((parts - 1,)),
            pltpu.SemaphoreType.DMA((parts - 1,)),
        ],
        compiler_params=pltpu.CompilerParams(
            collective_id=identity, has_side_effects=True, vmem_limit_bytes=60 * 1024 * 1024
        ),
        cost_estimate=pl.CostEstimate(
            flops=2 * rows * depth * columns * parts,
            bytes_accessed=2 * depth * columns * parts,
            transcendentals=0,
        ),
        name=f"project{identity}",
    )(attended, out_weight)


QUARTERS = 4
STREAMS = 4


def cut_bound(held_at):
    chips = range(4)
    loads = []
    for bit in (1, 2):
        for side in (0, bit):
            loads.append(
                sum(
                    held_at[c][d]
                    for c in chips
                    for d in chips
                    if c & bit == side and d & bit != side
                )
            )
    for c in chips:
        loads.append(sum(held_at[c][d] for d in chips if d != c))
        loads.append(sum(held_at[d][c] for d in chips if d != c))
    return max(-(-load // 2) for load in loads)


def left_hops(held_at):
    return sum(
        held_at[c][d] * (((c ^ d) & 1) + ((c ^ d) >> 1)) for c in range(4) for d in range(4)
    )


def try_moves(held_at, slots, rng, noise):
    held_at = [row[:] for row in held_at]
    moves = []
    for slot in range(slots):
        left = slots - slot
        hops = left_hops(held_at)
        if hops == 0:
            moves.append({})
            continue
        if hops > 8 * left or cut_bound(held_at) > left:
            return None
        free = [row[:] for row in held_at]
        chosen = {}
        links = [(c, link) for c in range(4) for link in (1, 2)]
        rng.shuffle(links)
        for c, link in links:
            best = None
            for d in range(4):
                if free[c][d] <= 0 or c == d:
                    continue
                if (c ^ d) == 3:
                    value = 2.0 + noise * rng.random()
                elif (c ^ d) & link:
                    value = 1.5 + 0.1 * free[c][d] + noise * rng.random()
                elif left >= 3 and free[c][d] > left - 1:
                    value = 0.5 + 1.5 * noise * rng.random()
                else:
                    continue
                if best is None or value > best[0]:
                    best = (value, d)
            if best:
                chosen[c, link] = best[1]
                free[c][best[1]] -= 1
        for (c, link), d in chosen.items():
            held_at[c][d] -= 1
            held_at[c ^ link][d] += 1
        moves.append(chosen)
    return moves if left_hops(held_at) == 0 else None


def find_moves(demand, rng, most):
    held_at = [[0] * 4 for _ in range(4)]
    for c in range(4):
        for d in demand[c]:
            held_at[c][d] += QUARTERS
    least = max(cut_bound(held_at), -(-left_hops(held_at) // 8))
    for slots in range(least, most + 1):
        for attempt in range(400):
            noise = 0.0 if attempt == 0 else (0.5 if attempt % 2 else 1.5)
            moves = try_moves(held_at, slots, rng, noise)
            if moves is not None:
                return slots, moves
    raise ValueError("no route")


def codes_of(demand, moves, most):
    ready = [[[] for _ in range(4)] for _ in range(4)]
    arriving = []
    for c in range(4):
        for place, d in enumerate(demand[c]):
            for k in range(QUARTERS):
                ready[c][d].append((place * QUARTERS + k, (c, place, k)))
    send = [[[0] * most for _ in range(2)] for _ in range(4)]
    for slot, chosen in enumerate(moves):
        arriving = []
        for (c, link), d in sorted(chosen.items()):
            code, chunk = ready[c][d].pop(0)
            send[c][link - 1][slot] = code
            arriving.append((c ^ link, d, 2 * QUARTERS + 2 * slot + link - 1, chunk))
        for c, d, code, chunk in arriving:
            ready[c][d].append((code, chunk))
    table = []
    for c in range(4):
        here = {chunk: code for code, chunk in ready[c][c]}
        items = sorted({chunk[:2] for chunk in here})
        finals = [here[item + (k,)] for item in items for k in range(QUARTERS)]
        table.append(send[c][0] + send[c][1] + finals)
    return table


@functools.lru_cache
def routes(most):
    pairs = [(a, b) for a in range(4) for b in range(a, 4)]
    rng = random.Random(1)
    place = np.zeros((len(pairs) ** 4,), np.int32)
    rows, slots = [], []
    for index, demand in enumerate(itertools.product(pairs, repeat=4)):
        flat = [d for pair in demand for d in pair]
        if any(flat.count(d) != 2 for d in range(4)):
            continue
        place[index] = len(rows)
        count, moves = find_moves(demand, rng, most)
        rows.append(codes_of(demand, moves, most))
        slots.append(count)
    return place, np.array(rows, np.int32), np.array(slots, np.int32)


def plan_kernel(
    lengths,
    moving,
    destination,
    place,
    rows,
    caches,
    plan,
    branch,
    held,
    found,
    line,
    buffer,
    sem,
    in_sem,
    out_sem,
    *,
    most,
):
    replicas = destination.shape[0]
    staying = 1 - moving[lax.axis_index("rep")]
    fetch_piece, put_piece, every = piece_copies(
        caches, staying, held, staying, buffer, in_sem, out_sem
    )
    for index in every:
        fetch_piece(*index).start()
    own = lax.axis_index("rep")
    chip = own // 2
    key = jnp.int32(0)
    swap = jnp.int32(0)
    for c in range(replicas // 2):
        first, second = destination[2 * c] // 2, destination[2 * c + 1] // 2
        low, high = jnp.minimum(first, second), jnp.maximum(first, second)
        key = key * 10 + low * (7 - low) // 2 + high
        swap = jnp.where(c == chip, (first > second).astype(jnp.int32), swap)
    seek = pltpu.make_async_copy(place.at[key // 128], found, sem)
    seek.start()
    anchor = jnp.int32(0)
    senders = [jnp.int32(0), jnp.int32(0)]
    for r in range(replicas):
        goal = destination[r]
        anchor = jnp.where(goal == own, r, anchor)
        senders = [
            jnp.where(goal == 2 * chip + index, r, sender)
            for index, sender in enumerate(senders)
        ]
    crossed = (senders[0] > senders[1]).astype(jnp.int32)
    leaving = moving[own]
    plan[0] = leaving
    at_slot = lax.broadcasted_iota(jnp.int32, lengths.shape, 0)
    at_row = lax.broadcasted_iota(jnp.int32, lengths.shape, 1)
    length_of = lengths[...].astype(jnp.float32)

    def look_up(row, slot):
        here = (at_row == row) & (at_slot == slot)
        return jnp.sum(jnp.where(here, length_of, 0.0)).astype(jnp.int32)

    plan[1] = look_up(own, 1 - leaving)
    plan[2] = look_up(anchor, moving[anchor])
    seek.wait()
    fetch = pltpu.make_async_copy(rows.at[found[0, key % 128]], line, sem)
    fetch.start()
    fetch.wait()
    branch[0] = line[0, line.shape[1] - 1]
    size = 2 * most + 2 * QUARTERS
    for index in range(size):
        at = index
        if index >= 2 * most:
            final = index - 2 * most
            at = 2 * most + (final + QUARTERS * crossed) % (2 * QUARTERS)
        code = line[0, chip * size + at]
        turned = (code + QUARTERS * swap) % (2 * QUARTERS)
        plan[4 + index] = jnp.where(code < 2 * QUARTERS, turned, code)
    for index in every:
        fetch_piece(*index).wait()
        put_piece(*index).start()
    for index in every:
        put_piece(*index).wait()


def piece_copies(source, source_slot, held, target_slot, buffer, in_sem, out_sem):
    pieces, halves = in_sem.shape
    size = buffer.shape[1] // pieces

    def fetch(piece, half):
        at = pl.ds(piece * size, size)
        return pltpu.make_async_copy(
            source.at[source_slot, half, at], buffer.at[half, at], in_sem.at[piece, half]
        )

    def put(piece, half):
        at = pl.ds(piece * size, size)
        return pltpu.make_async_copy(
            buffer.at[half, at], held.at[target_slot, half, at], out_sem.at[piece, half]
        )

    return fetch, put, list(itertools.product(range(pieces), range(halves)))


def make_plan(lengths, moving, destination, caches, counts):
    most = counts[-1]
    place, rows, slots = routes(most)
    lines = -(-place.size // 128)
    places = np.zeros((lines * 128,), np.int32)
    places[: place.size] = place
    table = np.zeros((rows.shape[0], 1, 128), np.int32)
    table[:, 0, : rows[0].size] = rows.reshape(rows.shape[0], -1)
    table[:, 0, 127] = np.sum(slots[:, None] > np.array(counts[:-1]), axis=1)
    anywhere = pl.BlockSpec(memory_space=pl.ANY)
    smem = pl.BlockSpec(memory_space=pltpu.SMEM)
    return pl.pallas_call(
        functools.partial(plan_kernel, most=most),
        out_shape=(
            jax.ShapeDtypeStruct((4 + 2 * most + 2 * QUARTERS,), jnp.int32),
            jax.ShapeDtypeStruct((1,), jnp.int32),
            jax.ShapeDtypeStruct(caches.shape, caches.dtype),
        ),
        in_specs=[
            pl.BlockSpec(memory_space=pltpu.VMEM),
            smem,
            smem,
            anywhere,
            anywhere,
            anywhere,
        ],
        out_specs=(smem, smem, anywhere),
        scratch_shapes=[
            pltpu.SMEM((1, 128), jnp.int32),
            pltpu.SMEM((1, 128), jnp.int32),
            pltpu.VMEM(caches.shape[1:], caches.dtype),
            pltpu.SemaphoreType.DMA,
            pltpu.SemaphoreType.DMA((4, caches.shape[1])),
            pltpu.SemaphoreType.DMA((4, caches.shape[1])),
        ],
        name="plan",
    )(
        lengths.T,
        moving,
        destination,
        jnp.asarray(places.reshape(lines, 1, 128)),
        jnp.asarray(table),
        caches,
    )


def route_kernel(
    plan,
    queries_from,
    keys_from,
    values_from,
    caches,
    weight,
    arrived,
    mixed,
    queries,
    keys_new,
    values_new,
    both,
    local,
    give,
    arr,
    stage,
    final,
    hand,
    query_t,
    row_max,
    row_total,
    weighted,
    attended,
    weight_blocks,
    outgoing,
    incoming,
    totals,
    fresh_sem,
    in_sem,
    give_sem,
    gave_sem,
    send_sem,
    recv_sem,
    keep_sem,
    hand_sem,
    got_sem,
    weight_sem,
    out_sem,
    mix_sem,
    *,
    slots,
    most,
):
    own = lax.axis_index("rep")
    part = lax.axis_index("tp")
    parts = weight_blocks.shape[0]
    core = own % 2
    partner = own + 1 - 2 * core
    across = (own + 2 - 4 * ((own // 2) % 2), own + 4 - 8 * (own // 4))
    rows = stage.shape[3]
    span, columns = mixed.shape[1:]
    kv_count = query_t.shape[0]
    group = query_t.shape[2] // span
    run = QUARTERS * rows
    factor = HEAD ** (-0.5) * LOG2E
    leaving = plan[0]

    def fetch(s):
        return pltpu.make_async_copy(
            caches.at[:, :, pl.ds(s * run, run)], both.at[s], in_sem.at[s]
        )

    def load(step):
        at = pl.ds(pl.multiple_of(lax.rem(part + step, parts) * columns, columns), columns)
        return pltpu.make_async_copy(
            weight.at[:, at], weight_blocks.at[step], weight_sem.at[step]
        )

    fresh_copies = [
        pltpu.make_async_copy(source, into, fresh_sem.at[index])
        for index, (source, into) in enumerate(
            ((queries_from, queries), (keys_from, keys_new), (values_from, values_new))
        )
    ]
    for s in range(STREAMS):
        fetch(s).start()
    barrier = pltpu.get_barrier_semaphore()
    peers = [{"rep": partner}] + [{"rep": peer} for peer in across]
    peers += [{"tp": lax.rem(part + step, parts)} for step in range(1, parts)]
    for peer in peers:
        pl.semaphore_signal(
            barrier, inc=1, device_id=peer, device_id_type=pl.DeviceIdType.MESH
        )

    def remote(src, dst, send, recv, peer):
        return pltpu.make_async_remote_copy(
            src_ref=src,
            dst_ref=dst,
            send_sem=send,
            recv_sem=recv,
            device_id=peer,
            device_id_type=pl.DeviceIdType.MESH,
        )

    def share(s):
        return remote(
            give.at[s],
            local.at[s, pl.ds(core * QUARTERS, QUARTERS)],
            give_sem.at[s],
            gave_sem.at[s],
            {"rep": partner},
        )

    def send(link, slot, s):
        return remote(
            stage.at[link, slot, s],
            arr.at[link, slot, s],
            send_sem.at[link, slot, s],
            recv_sem.at[link, slot, s],
            {"rep": across[link]},
        )

    def settle(s, half):
        return pltpu.make_async_copy(
            final.at[s, half],
            arrived.at[0, half, pl.ds(s * run, run)],
            keep_sem.at[s, half],
        )

    def deliver(s):
        return remote(
            hand.at[s],
            final.at[s, core],
            hand_sem.at[s],
            got_sem.at[s],
            {"rep": partner},
        )

    def mix(kind, index, place, target):
        return remote(
            outgoing.at[kind, index],
            incoming.at[kind, place],
            out_sem.at[kind, index],
            mix_sem.at[kind, place],
            {"tp": target},
        )

    def pick(s, upto, codes, write):
        def body(block, carry):
            at = pl.ds(pl.multiple_of(block * BLOCK_ROWS, BLOCK_ROWS), BLOCK_ROWS)
            values = [local[s, 0, at]] * len(codes)
            came = [(home, local[s, home, at]) for home in range(1, 2 * QUARTERS)]
            came += [
                (2 * QUARTERS + 2 * slot + link, arr[link, slot, s, at])
                for slot in range(upto)
                for link in range(2)
            ]
            for here, piece in came:
                values = [
                    lax.select(code == here, piece, value)
                    for code, value in zip(codes, values)
                ]
            for index, value in enumerate(values):
                write(index, block, value)
            return carry

        lax.fori_loop(0, rows // BLOCK_ROWS, body, 0)

    def share_out(s, carry):
        fetch(s).wait()

        def body(block, carry):
            k = block // (rows // BLOCK_ROWS)
            inner = pl.multiple_of(block % (rows // BLOCK_ROWS) * BLOCK_ROWS, BLOCK_ROWS)
            at = pl.ds(pl.multiple_of(block * BLOCK_ROWS, BLOCK_ROWS), BLOCK_ROWS)
            to = pl.ds(inner, BLOCK_ROWS)
            for half, into in ((1 - core, None), (core, core)):
                value = lax.select(
                    leaving == 0, both[s, 0, half, at], both[s, 1, half, at]
                )
                if into is None:
                    give[s, k, to] = value
                else:
                    local[s, core * QUARTERS + k, to] = value
            return carry

        lax.fori_loop(0, run // BLOCK_ROWS, body, 0)

        @pl.when(s == 0)
        def _():
            pl.semaphore_wait(barrier, len(peers))

        share(s).start()

        return carry

    lax.fori_loop(0, STREAMS, share_out, 0)
    for copy in fresh_copies:
        copy.start()
    for step in list(range(1, parts)) + [0]:
        load(step).start()

    def lanes_of(head):
        return slice(head * HEAD, (head + 1) * HEAD)

    def mix_values(values, weights):
        return lax.dot_general(
            values,
            weights.astype(jnp.bfloat16),
            (((0,), (0,)), ((), ())),
            preferred_element_type=jnp.float32,
        )

    def scores_of(head, keys):
        return lax.dot_general(
            keys,
            query_t[head],
            (((1,), (0,)), ((), ())),
            preferred_element_type=jnp.float32,
        )

    def fresh(slot):
        def choose(ref, lanes):
            return lax.select(slot == 0, ref[0, :, lanes], ref[1, :, lanes])

        key_at = lax.broadcasted_iota(jnp.int32, (span, group * span), 0)
        token_at = lax.broadcasted_iota(jnp.int32, (span, group * span), 1) % span
        for head in range(kv_count):
            for member in range(group):
                query_t[head, :, member * span : (member + 1) * span] = choose(
                    queries, lanes_of(head * group + member)
                ).T
            scores = jnp.where(
                key_at <= token_at, scores_of(head, choose(keys_new, lanes_of(head))), masked_score
            )
            new_max = jnp.max(scores, axis=0, keepdims=True)
            weights = jnp.exp2((scores - new_max) * factor)
            row_max[head] = new_max
            row_total[head] = jnp.sum(weights, axis=0, keepdims=True)
            weighted[head] = mix_values(choose(values_new, lanes_of(head)), weights)

    def absorb(start, length, piece):
        every = [scores_of(head, piece(0, head)) for head in range(kv_count)]
        for head, scores in enumerate(every):
            parts_of = [
                scores[at : at + LENGTH_STEP]
                + jnp.where(start + at < length, 0.0, masked_score)
                for at in range(0, scores.shape[0], LENGTH_STEP)
            ]
            old_max = row_max[head]
            new_max = old_max
            for some in parts_of:
                new_max = jnp.maximum(new_max, jnp.max(some, axis=0, keepdims=True))
            rescale = jnp.exp2((old_max - new_max) * factor)
            weights = [jnp.exp2((some - new_max) * factor) for some in parts_of]
            row_max[head] = new_max
            total = row_total[head] * rescale
            for some in weights:
                total = total + jnp.sum(some, axis=0, keepdims=True)
            row_total[head] = total
            rounded = jnp.concatenate([some.astype(jnp.bfloat16) for some in weights], axis=0)
            weighted[head] = weighted[head] * rescale + mix_values(piece(1, head), rounded)

    def finish():
        for head in range(kv_count):
            result = (weighted[head] / row_total[head]).T
            for member in range(group):
                attended[:, lanes_of(head * group + member)] = result[
                    member * span : (member + 1) * span
                ].astype(jnp.bfloat16)

    relayed = parts == 4
    low = part < parts // 2
    edge = (part == 0) | (part == parts - 1)

    def mirror(place):
        return jnp.where(low, place, parts - 1 - place)

    def product(column):
        step = lax.rem(column - part + parts, parts)
        return jnp.dot(
            attended[...], weight_blocks[step], preferred_element_type=jnp.float32
        )

    def spread_direct(kind):
        def body(index, carry):
            column = lax.rem(part + 1 + index, parts)
            if kind == 0:
                load(lax.rem(index + 1, parts)).wait()
            value = product(column)

            @pl.when(index < parts - 1)
            def _():
                outgoing[kind, index] = value.astype(jnp.bfloat16)
                mix(kind, index, part, column).start()

            @pl.when(index == parts - 1)
            def _():
                totals[kind] = value

            return carry

        lax.fori_loop(0, parts, body, 0)

    def collect_direct(kind):
        for step in range(1, parts):
            place = lax.rem(part + step, parts)
            mix(kind, 0, place, place).wait_recv()
            totals[kind] += incoming[kind, place].astype(jnp.float32)

    def spread_relayed(kind):
        def body(index, carry):
            goal = jnp.where(
                edge,
                jnp.where(index < 2, 3 - index, jnp.where(index == 2, 0, 1)),
                jnp.where(index == 0, 2, jnp.where(index == 1, 0, index * 2 - 3)),
            )
            value = product(mirror(goal))
            slot = jnp.where(index < 2, index, 2)

            @pl.when(index == 2)
            def _():
                totals[kind] = value

            @pl.when((index != 2) & ((index < 3) | edge))
            def _():
                outgoing[kind, slot] = value.astype(jnp.bfloat16)

            @pl.when((index == 3) & jnp.logical_not(edge))
            def _():
                mix(kind, 2, parts, part).wait_recv()
                outgoing[kind, slot] = (
                    value + incoming[kind, parts].astype(jnp.float32)
                ).astype(jnp.bfloat16)

            @pl.when(index != 2)
            def _():
                first = edge & (index == 0)
                mix(
                    kind,
                    slot,
                    jnp.where(first, parts, part),
                    mirror(jnp.where(first, 1, goal)),
                ).start()

            return carry

        lax.fori_loop(0, parts, body, 0)

    def collect_relayed(kind):
        def take(place):
            mix(kind, 0, mirror(place), part).wait_recv()
            totals[kind] += incoming[kind, mirror(place)].astype(jnp.float32)

        @pl.when(edge)
        def _():
            take(1)

        @pl.when(jnp.logical_not(edge))
        def _():
            take(0)
            take(3)

        take(2)

    spread_arrived = spread_relayed if relayed else spread_direct
    collect_arrived = collect_relayed if relayed else collect_direct

    staying_blocks = run // BLOCK

    def absorb_staying(s, block):
        inner = pl.multiple_of(block * BLOCK, BLOCK)
        at = pl.ds(inner, BLOCK)

        def piece(half, head):
            return lax.select(
                leaving == 0,
                both[s, 1, half, at, lanes_of(head)],
                both[s, 0, half, at, lanes_of(head)],
            )

        absorb(s * run + inner, plan[1], piece)

    for slot in range(slots):
        codes = [plan[4 + link * most + slot] for link in range(2)]

        def step_of(s, carry):
            if slot == 0:
                share(s).wait_recv()
            else:
                for link in range(2):
                    send(link, slot - 1, s).wait_recv()

            def write(link, block, value):
                at = pl.ds(pl.multiple_of(block * BLOCK_ROWS, BLOCK_ROWS), BLOCK_ROWS)
                stage[link, slot, s, at] = value

            pick(s, slot, codes, write)
            for link in range(2):
                send(link, slot, s).start()
            if 1 <= slot <= staying_blocks:
                absorb_staying(s, slot - 1)
            return carry

        lax.fori_loop(0, STREAMS, step_of, 0)
        if slot == 0:
            for copy in fresh_copies:
                copy.wait()
            fresh(1 - leaving)
        if slot == staying_blocks:
            finish()
            spread_direct(0)
            fresh(leaving)

    def last_step(s, carry):
        @pl.when(s < STREAMS)
        def _():
            for link in range(2):
                send(link, slots - 1, s).wait_recv()
            for k in range(QUARTERS):
                base = 4 + 2 * most + k
                codes = [plan[base + QUARTERS * core], plan[base + QUARTERS * (1 - core)]]

                def write(index, block, value):
                    at = pl.ds(
                        pl.multiple_of(k * rows + block * BLOCK_ROWS, BLOCK_ROWS), BLOCK_ROWS
                    )
                    if index == 0:
                        final[s, core, at] = value
                    else:
                        hand[s, at] = value

                pick(s, slots, codes, write)
            deliver(s).start()

        @pl.when(s > 0)
        def _():
            before = s - 1
            deliver(before).wait_recv()
            for half in range(2):
                settle(before, half).start()

            def body(block, carry):
                inner = pl.multiple_of(block * BLOCK, BLOCK)
                at = pl.ds(inner, BLOCK)
                absorb(
                    before * run + inner,
                    plan[2],
                    lambda half, head: final[before, half, at, lanes_of(head)],
                )
                return carry

            lax.fori_loop(0, staying_blocks, body, 0)

        return carry

    lax.fori_loop(0, STREAMS + 1, last_step, 0)
    finish()
    spread_arrived(1)
    collect_direct(0)
    staying_mixed = totals[0].astype(jnp.bfloat16)
    collect_arrived(1)
    arrived_mixed = totals[1].astype(jnp.bfloat16)
    mixed[0] = lax.select(leaving == 0, arrived_mixed, staying_mixed)
    mixed[1] = lax.select(leaving == 0, staying_mixed, arrived_mixed)
    for kind in range(2):
        for index in range(parts - 1):
            mix(kind, index, part, lax.rem(part + 1, parts)).wait_send()

    def drain(s, carry):
        share(s).wait_send()
        for slot in range(slots):
            for link in range(2):
                send(link, slot, s).wait_send()
        for half in range(2):
            settle(s, half).wait()
        deliver(s).wait_send()
        return carry

    lax.fori_loop(0, STREAMS, drain, 0)


def route(plan, queries, keys_new, values_new, caches, out_weight, slots, most, identity):
    parts = lax.axis_size("tp")
    slot_count, span, features = queries.shape
    depth = out_weight.shape[0]
    columns = out_weight.shape[1] // parts
    halves, cache_rows, width = caches.shape[1:]
    run = cache_rows // STREAMS
    rows = run // QUARTERS
    kv_count = width // HEAD
    grouped = span * features // width
    anywhere = pl.BlockSpec(memory_space=pl.ANY)
    vmem = pl.BlockSpec(memory_space=pltpu.VMEM)
    kind = jnp.bfloat16
    dma = pltpu.SemaphoreType.DMA
    scratch = [
        pltpu.VMEM(queries.shape, kind),
        pltpu.VMEM(keys_new.shape, kind),
        pltpu.VMEM(values_new.shape, kind),
        pltpu.VMEM((STREAMS, slot_count, halves, run, width), kind),
        pltpu.VMEM((STREAMS, 2 * QUARTERS, rows, width), kind),
        pltpu.VMEM((STREAMS, QUARTERS, rows, width), kind),
        pltpu.VMEM((2, slots, STREAMS, rows, width), kind),
        pltpu.VMEM((2, slots, STREAMS, rows, width), kind),
        pltpu.VMEM((STREAMS, halves, run, width), kind),
        pltpu.VMEM((STREAMS, run, width), kind),
        pltpu.VMEM((kv_count, HEAD, grouped), kind),
        pltpu.VMEM((kv_count, 1, grouped), jnp.float32),
        pltpu.VMEM((kv_count, 1, grouped), jnp.float32),
        pltpu.VMEM((kv_count, HEAD, grouped), jnp.float32),
        pltpu.VMEM((span, features), kind),
        pltpu.VMEM((parts, depth, columns), kind),
        pltpu.VMEM((2, parts - 1, span, columns), kind),
        pltpu.VMEM((2, parts + 1, span, columns), kind),
        pltpu.VMEM((2, span, columns), jnp.float32),
        dma((3,)),
        dma((STREAMS,)),
        dma((STREAMS,)),
        dma((STREAMS,)),
        dma((2, slots, STREAMS)),
        dma((2, slots, STREAMS)),
        dma((STREAMS, halves)),
        dma((STREAMS,)),
        dma((STREAMS,)),
        dma((parts,)),
        dma((2, parts - 1)),
        dma((2, parts + 1)),
    ]
    return pl.pallas_call(
        functools.partial(route_kernel, slots=slots, most=most),
        out_shape=(
            jax.ShapeDtypeStruct((1, halves, cache_rows, width), kind),
            jax.ShapeDtypeStruct((slot_count, span, columns), kind),
        ),
        in_specs=[pl.BlockSpec(memory_space=pltpu.SMEM)] + [anywhere] * 5,
        out_specs=(anywhere, vmem),
        scratch_shapes=scratch,
        compiler_params=pltpu.CompilerParams(
            collective_id=identity, has_side_effects=True, vmem_limit_bytes=60 * 1024 * 1024
        ),
        name=f"route{slots}",
    )(plan, queries, keys_new, values_new, caches, out_weight)


def hold_kernel(plan, arrived, mixed, _, out, held, buffer, in_sem, out_sem):
    leaving = plan[0]
    fetch, put, every = piece_copies(arrived, 0, held, leaving, buffer, in_sem, out_sem)
    for index in every:
        fetch(*index).start()
    out[...] = mixed[...]
    for index in every:
        fetch(*index).wait()
        put(*index).start()
    for index in every:
        put(*index).wait()


def hold(plan, arrived, mixed, held):
    anywhere = pl.BlockSpec(memory_space=pl.ANY)
    vmem = pl.BlockSpec(memory_space=pltpu.VMEM)
    return pl.pallas_call(
        hold_kernel,
        out_shape=(
            jax.ShapeDtypeStruct(mixed.shape, mixed.dtype),
            jax.ShapeDtypeStruct(held.shape, held.dtype),
        ),
        in_specs=[pl.BlockSpec(memory_space=pltpu.SMEM), anywhere, vmem, anywhere],
        out_specs=(vmem, anywhere),
        scratch_shapes=[
            pltpu.VMEM(held.shape[1:], held.dtype),
            pltpu.SemaphoreType.DMA((4, held.shape[1])),
            pltpu.SemaphoreType.DMA((4, held.shape[1])),
        ],
        input_output_aliases={3: 1},
        name="hold",
    )(plan, arrived, mixed, held)


def migrate(queries, keys_new, values_new, caches, lengths, moving, destination, out_weight):
    slot_count = caches.shape[0]
    span = queries.shape[0] // slot_count
    counts = (4, 5, 6, 8)
    plan, branch, held = make_plan(lengths, moving, destination, caches, counts)

    def by_slot(array):
        return array.reshape(slot_count, span, array.shape[1])

    arrived, mixed = lax.switch(
        branch[0],
        [
            functools.partial(route, slots=slots, most=counts[-1], identity=2 + index)
            for index, slots in enumerate(counts)
        ],
        plan,
        by_slot(queries),
        by_slot(keys_new),
        by_slot(values_new),
        caches,
        out_weight,
    )
    mixed, held = hold(plan, arrived, mixed, held)
    return mixed.reshape(slot_count * span, mixed.shape[2]), held


def on_device(queries, keys_new, values_new, caches, lengths, moving, destination, out_weight):
    replicas = lax.axis_size("rep")
    if replicas == 8:
        return migrate(
            queries, keys_new, values_new, caches, lengths, moving, destination, out_weight
        )
    own_index = lax.axis_index("rep")
    slot_count, _, cache_rows, width = caches.shape
    span = queries.shape[0] // slot_count
    kv_count = width // HEAD
    group = queries.shape[1] // width
    leaving_slot = moving[own_index]
    staying_slot = 1 - leaving_slot
    every = jnp.arange(replicas, dtype=jnp.int32)
    source_of = jnp.sum(
        jnp.where(destination[None, :] == every[:, None], every[None, :], 0), axis=1
    )
    anchor = source_of[own_index]
    incoming_length = lengths[anchor, moving[anchor]]
    staying_length = lengths[own_index, staying_slot]
    query_t = (
        queries.reshape(slot_count, span, kv_count, group, HEAD)
        .transpose(0, 2, 4, 3, 1)
        .reshape(slot_count, kv_count, HEAD, group * span)
    )
    keys_by_slot = keys_new.reshape(slot_count, span, width)
    values_by_slot = values_new.reshape(slot_count, span, width)

    def pick(array, slot):
        return lax.dynamic_index_in_dim(array, slot, 0, keepdims=False)

    held, staying_attended = attend_slot(
        jnp.stack([staying_slot, staying_slot, staying_length]),
        caches,
        pick(query_t, staying_slot),
        pick(keys_by_slot, staying_slot),
        pick(values_by_slot, staying_slot),
        None,
        caches.shape,
    )
    leaving = lax.dynamic_index_in_dim(caches, leaving_slot, 0, keepdims=False)
    piece_rows = 2 * cache_rows // replicas
    pieces = leaving.reshape(replicas, piece_rows, width)
    spread = lax.all_to_all(pieces, "rep", split_axis=0, concat_axis=0, tiled=True)
    ordered = jnp.take(spread, source_of, axis=0, mode="clip")
    arrived = lax.all_to_all(ordered, "rep", split_axis=0, concat_axis=0, tiled=True)
    arrived = arrived.reshape(1, 2, cache_rows, width)
    staying_mixed = project(staying_attended, out_weight, 0)
    held, arrived_attended = attend_slot(
        jnp.stack([jnp.zeros_like(leaving_slot), leaving_slot, incoming_length]),
        arrived,
        pick(query_t, leaving_slot),
        pick(keys_by_slot, leaving_slot),
        pick(values_by_slot, leaving_slot),
        held,
        caches.shape,
    )
    arrived_mixed = project(arrived_attended, out_weight, 1)
    mixed = jnp.where(
        leaving_slot == 0,
        jnp.concatenate([arrived_mixed, staying_mixed], axis=0),
        jnp.concatenate([staying_mixed, arrived_mixed], axis=0),
    )
    return (mixed, held)


def solution(mesh):
    in_specs = (
        P("rep", "tp"),
        P("rep", "tp"),
        P("rep", "tp"),
        P("rep", None, None, "tp"),
        P(),
        P(),
        P(),
        P("tp", None),
    )
    out_specs = (P("rep", "tp"), P("rep", None, None, "tp"))
    return jax.shard_map(
        on_device, mesh=mesh, in_specs=in_specs, out_specs=out_specs, check_vma=False
    )
```

```python
import functools
import itertools
import random

import jax
import jax.numpy as jnp
import numpy as np
from jax import lax
from jax.experimental import pallas as pl
from jax.experimental.pallas import tpu as pltpu
from jax.sharding import PartitionSpec as P

HEAD = 128
BLOCK = 512
LOG2E = 1.4426950408889634
masked_score = -1e30
BLOCK_ROWS = 64
LENGTH_STEP = 128
PIECES = 2


def slot_kernel(
    scalars, source, query_t, keys_fresh, values_fresh, *rest, aliased, kv_count, group
):
    if aliased:
        rest = rest[1:]
    held, attended, cache, row_max, row_total, weighted, in_sem, out_sem = rest
    taken, target, length = scalars[0], scalars[1], scalars[2]
    rows = cache.shape[1]
    blocks = rows // BLOCK
    span = keys_fresh.shape[0]
    factor = HEAD ** (-0.5) * LOG2E

    def fetch(block, part):
        at = pl.ds(pl.multiple_of(block * BLOCK, BLOCK), BLOCK)
        return pltpu.make_async_copy(
            source.at[taken, part, at], cache.at[part, at], in_sem.at[block, part]
        )

    def put(block, part):
        at = pl.ds(pl.multiple_of(block * BLOCK, BLOCK), BLOCK)
        return pltpu.make_async_copy(
            cache.at[part, at], held.at[target, part, at], out_sem.at[block, part]
        )

    for block in range(blocks):
        for part in range(2):
            fetch(block, part).start()

    def scores_of(head, keys):
        return lax.dot_general(
            keys,
            query_t[head],
            (((1,), (0,)), ((), ())),
            preferred_element_type=jnp.float32,
        )

    def mix(values, weights):
        return lax.dot_general(
            values,
            weights.astype(jnp.bfloat16),
            (((0,), (0,)), ((), ())),
            preferred_element_type=jnp.float32,
        )

    key_at = lax.broadcasted_iota(jnp.int32, (span, group * span), 0)
    token_at = lax.broadcasted_iota(jnp.int32, (span, group * span), 1) % span
    for head in range(kv_count):
        lanes = slice(head * HEAD, (head + 1) * HEAD)
        scores = jnp.where(
            key_at <= token_at, scores_of(head, keys_fresh[:, lanes]), masked_score
        )
        new_max = jnp.max(scores, axis=0, keepdims=True)
        weights = jnp.exp2((scores - new_max) * factor)
        row_max[head] = new_max
        row_total[head] = jnp.sum(weights, axis=0, keepdims=True)
        weighted[head] = mix(values_fresh[:, lanes], weights)

    def absorb(block, masked):
        start = pl.multiple_of(block * BLOCK, BLOCK)
        at = pl.ds(start, BLOCK)
        for head in range(kv_count):
            lanes = slice(head * HEAD, (head + 1) * HEAD)
            scores = scores_of(head, cache[0, at, lanes])
            if masked:
                position = start + lax.broadcasted_iota(jnp.int32, scores.shape, 0)
                scores = jnp.where(position < length, scores, masked_score)
            old_max = row_max[head]
            new_max = jnp.maximum(old_max, jnp.max(scores, axis=0, keepdims=True))
            rescale = jnp.exp2((old_max - new_max) * factor)
            weights = jnp.exp2((scores - new_max) * factor)
            row_max[head] = new_max
            row_total[head] = row_total[head] * rescale + jnp.sum(
                weights, axis=0, keepdims=True
            )
            weighted[head] = weighted[head] * rescale + mix(cache[1, at, lanes], weights)

    def step(block, carry):
        for part in range(2):
            fetch(block, part).wait()
            put(block, part).start()
        start = block * BLOCK

        @pl.when(start + BLOCK <= length)
        def _():
            absorb(block, False)

        @pl.when((start < length) & (length < start + BLOCK))
        def _():
            absorb(block, True)

        return carry

    lax.fori_loop(0, blocks, step, 0)
    for head in range(kv_count):
        result = (weighted[head] / row_total[head]).T
        for member in range(group):
            lanes = slice((head * group + member) * HEAD, (head * group + member + 1) * HEAD)
            attended[:, lanes] = result[member * span : (member + 1) * span].astype(
                jnp.bfloat16
            )
    for block in range(blocks):
        for part in range(2):
            put(block, part).wait()


def attend_slot(scalars, source, query_t, keys_fresh, values_fresh, held, held_shape):
    kv_count, _, columns = query_t.shape
    span = keys_fresh.shape[0]
    group = columns // span
    rows, width = source.shape[2:]
    aliased = held is not None
    anywhere = pl.BlockSpec(memory_space=pl.ANY)
    vmem = pl.BlockSpec(memory_space=pltpu.VMEM)
    operands = [scalars, source, query_t, keys_fresh, values_fresh]
    in_specs = [pl.BlockSpec(memory_space=pltpu.SMEM), anywhere, vmem, vmem, vmem]
    if aliased:
        operands.append(held)
        in_specs.append(anywhere)
    blocks = rows // BLOCK
    return pl.pallas_call(
        functools.partial(slot_kernel, aliased=aliased, kv_count=kv_count, group=group),
        out_shape=(
            jax.ShapeDtypeStruct(held_shape, jnp.bfloat16),
            jax.ShapeDtypeStruct((span, kv_count * group * HEAD), jnp.bfloat16),
        ),
        in_specs=in_specs,
        out_specs=(anywhere, vmem),
        scratch_shapes=[
            pltpu.VMEM((2, rows, width), jnp.bfloat16),
            pltpu.VMEM((kv_count, 1, columns), jnp.float32),
            pltpu.VMEM((kv_count, 1, columns), jnp.float32),
            pltpu.VMEM((kv_count, HEAD, columns), jnp.float32),
            pltpu.SemaphoreType.DMA((blocks, 2)),
            pltpu.SemaphoreType.DMA((blocks, 2)),
        ],
        input_output_aliases={5: 0} if aliased else {},
        compiler_params=pltpu.CompilerParams(vmem_limit_bytes=60 * 1024 * 1024),
        cost_estimate=pl.CostEstimate(
            flops=4 * kv_count * columns * (rows + span) * HEAD,
            bytes_accessed=8 * rows * width,
            transcendentals=kv_count * columns * (rows + span),
        ),
    )(*operands)


def project_kernel(
    attended, weight, out, weight_blocks, outgoing, incoming, weight_sem, send_sem, recv_sem
):
    parts = weight_blocks.shape[0]
    own = lax.axis_index("tp")
    columns = out.shape[1]

    def load(step):
        part = lax.rem(own + step, parts)
        at = pl.ds(pl.multiple_of(part * columns, columns), columns)
        return pltpu.make_async_copy(
            weight.at[:, at], weight_blocks.at[step], weight_sem.at[step]
        )

    order = list(range(1, parts)) + [0]
    for step in order:
        load(step).start()
    barrier = pltpu.get_barrier_semaphore()
    for step in range(1, parts):
        pl.semaphore_signal(
            barrier,
            inc=1,
            device_id={"tp": lax.rem(own + step, parts)},
            device_id_type=pl.DeviceIdType.MESH,
        )

    def product(step):
        load(step).wait()
        return jnp.dot(
            attended[...], weight_blocks[step], preferred_element_type=jnp.float32
        )

    copies = []
    for step in range(1, parts):
        outgoing[step - 1] = product(step).astype(jnp.bfloat16)
        if step == 1:
            pl.semaphore_wait(barrier, parts - 1)
        copy = pltpu.make_async_remote_copy(
            src_ref=outgoing.at[step - 1],
            dst_ref=incoming.at[step - 1],
            send_sem=send_sem.at[step - 1],
            recv_sem=recv_sem.at[step - 1],
            device_id={"tp": lax.rem(own + step, parts)},
            device_id_type=pl.DeviceIdType.MESH,
        )
        copy.start()
        copies.append(copy)
    total = product(0)
    for step, copy in enumerate(copies):
        copy.wait_recv()
        total = total + incoming[step].astype(jnp.float32)
    out[...] = total.astype(jnp.bfloat16)
    for copy in copies:
        copy.wait_send()


def project(attended, out_weight, identity):
    parts = lax.axis_size("tp")
    rows, depth = attended.shape
    columns = out_weight.shape[1] // parts
    vmem = pl.BlockSpec(memory_space=pltpu.VMEM)
    return pl.pallas_call(
        project_kernel,
        out_shape=jax.ShapeDtypeStruct((rows, columns), jnp.bfloat16),
        in_specs=[vmem, pl.BlockSpec(memory_space=pl.ANY)],
        out_specs=vmem,
        scratch_shapes=[
            pltpu.VMEM((parts, depth, columns), jnp.bfloat16),
            pltpu.VMEM((parts - 1, rows, columns), jnp.bfloat16),
            pltpu.VMEM((parts - 1, rows, columns), jnp.bfloat16),
            pltpu.SemaphoreType.DMA((parts,)),
            pltpu.SemaphoreType.DMA((parts - 1,)),
            pltpu.SemaphoreType.DMA((parts - 1,)),
        ],
        compiler_params=pltpu.CompilerParams(
            collective_id=identity, has_side_effects=True, vmem_limit_bytes=60 * 1024 * 1024
        ),
        cost_estimate=pl.CostEstimate(
            flops=2 * rows * depth * columns * parts,
            bytes_accessed=2 * depth * columns * parts,
            transcendentals=0,
        ),
        name=f"project{identity}",
    )(attended, out_weight)


QUARTERS = 4
STREAMS = 8


def cut_bound(held_at):
    chips = range(4)
    loads = []
    for bit in (1, 2):
        for side in (0, bit):
            loads.append(
                sum(
                    held_at[c][d]
                    for c in chips
                    for d in chips
                    if c & bit == side and d & bit != side
                )
            )
    for c in chips:
        loads.append(sum(held_at[c][d] for d in chips if d != c))
        loads.append(sum(held_at[d][c] for d in chips if d != c))
    return max(-(-load // 2) for load in loads)


def left_hops(held_at):
    return sum(
        held_at[c][d] * (((c ^ d) & 1) + ((c ^ d) >> 1)) for c in range(4) for d in range(4)
    )


def try_moves(held_at, slots, rng, noise):
    held_at = [row[:] for row in held_at]
    moves = []
    for slot in range(slots):
        left = slots - slot
        hops = left_hops(held_at)
        if hops == 0:
            moves.append({})
            continue
        if hops > 8 * left or cut_bound(held_at) > left:
            return None
        free = [row[:] for row in held_at]
        chosen = {}
        links = [(c, link) for c in range(4) for link in (1, 2)]
        rng.shuffle(links)
        for c, link in links:
            best = None
            for d in range(4):
                if free[c][d] <= 0 or c == d:
                    continue
                if (c ^ d) == 3:
                    value = 2.0 + noise * rng.random()
                elif (c ^ d) & link:
                    value = 1.5 + 0.1 * free[c][d] + noise * rng.random()
                elif left >= 3 and free[c][d] > left - 1:
                    value = 0.5 + 1.5 * noise * rng.random()
                else:
                    continue
                if best is None or value > best[0]:
                    best = (value, d)
            if best:
                chosen[c, link] = best[1]
                free[c][best[1]] -= 1
        for (c, link), d in chosen.items():
            held_at[c][d] -= 1
            held_at[c ^ link][d] += 1
        moves.append(chosen)
    return moves if left_hops(held_at) == 0 else None


def find_moves(demand, rng, most):
    held_at = [[0] * 4 for _ in range(4)]
    for c in range(4):
        for d in demand[c]:
            held_at[c][d] += QUARTERS
    least = max(cut_bound(held_at), -(-left_hops(held_at) // 8))
    for slots in range(least, most + 1):
        for attempt in range(400):
            noise = 0.0 if attempt == 0 else (0.5 if attempt % 2 else 1.5)
            moves = try_moves(held_at, slots, rng, noise)
            if moves is not None:
                return slots, moves
    raise ValueError("no route")


def codes_of(demand, moves, most):
    ready = [[[] for _ in range(4)] for _ in range(4)]
    arriving = []
    for c in range(4):
        for place, d in enumerate(demand[c]):
            for k in range(QUARTERS):
                ready[c][d].append((place * QUARTERS + k, (c, place, k)))
    send = [[[0] * most for _ in range(2)] for _ in range(4)]
    for slot, chosen in enumerate(moves):
        arriving = []
        for (c, link), d in sorted(chosen.items()):
            code, chunk = ready[c][d].pop(0)
            send[c][link - 1][slot] = code
            arriving.append((c ^ link, d, 2 * QUARTERS + 2 * slot + link - 1, chunk))
        for c, d, code, chunk in arriving:
            ready[c][d].append((code, chunk))
    table = []
    for c in range(4):
        here = {chunk: code for code, chunk in ready[c][c]}
        items = sorted({chunk[:2] for chunk in here})
        finals = [here[item + (k,)] for item in items for k in range(QUARTERS)]
        table.append(send[c][0] + send[c][1] + finals)
    return table


@functools.lru_cache
def routes(most):
    pairs = [(a, b) for a in range(4) for b in range(a, 4)]
    rng = random.Random(1)
    place = np.zeros((len(pairs) ** 4,), np.int32)
    rows, slots = [], []
    for index, demand in enumerate(itertools.product(pairs, repeat=4)):
        flat = [d for pair in demand for d in pair]
        if any(flat.count(d) != 2 for d in range(4)):
            continue
        place[index] = len(rows)
        count, moves = find_moves(demand, rng, most)
        rows.append(codes_of(demand, moves, most))
        slots.append(count)
    return place, np.array(rows, np.int32), np.array(slots, np.int32)


def plan_kernel(
    lengths,
    moving,
    destination,
    place,
    rows,
    caches,
    plan,
    branch,
    held,
    found,
    line,
    buffer,
    sem,
    in_sem,
    out_sem,
    *,
    most,
):
    replicas = destination.shape[0]
    staying = 1 - moving[lax.axis_index("rep")]
    fetch_piece, put_piece, every = piece_copies(
        caches, staying, held, staying, buffer, in_sem, out_sem
    )
    for index in every:
        fetch_piece(*index).start()
    own = lax.axis_index("rep")
    chip = own // 2
    key = jnp.int32(0)
    swap = jnp.int32(0)
    for c in range(replicas // 2):
        first, second = destination[2 * c] // 2, destination[2 * c + 1] // 2
        low, high = jnp.minimum(first, second), jnp.maximum(first, second)
        key = key * 10 + low * (7 - low) // 2 + high
        swap = jnp.where(c == chip, (first > second).astype(jnp.int32), swap)
    seek = pltpu.make_async_copy(place.at[key // 128], found, sem)
    seek.start()
    anchor = jnp.int32(0)
    senders = [jnp.int32(0), jnp.int32(0)]
    for r in range(replicas):
        goal = destination[r]
        anchor = jnp.where(goal == own, r, anchor)
        senders = [
            jnp.where(goal == 2 * chip + index, r, sender)
            for index, sender in enumerate(senders)
        ]
    crossed = (senders[0] > senders[1]).astype(jnp.int32)
    leaving = moving[own]
    plan[0] = leaving
    at_slot = lax.broadcasted_iota(jnp.int32, lengths.shape, 0)
    at_row = lax.broadcasted_iota(jnp.int32, lengths.shape, 1)
    length_of = lengths[...].astype(jnp.float32)

    def look_up(row, slot):
        here = (at_row == row) & (at_slot == slot)
        return jnp.sum(jnp.where(here, length_of, 0.0)).astype(jnp.int32)

    plan[1] = look_up(own, 1 - leaving)
    plan[2] = look_up(anchor, moving[anchor])
    seek.wait()
    fetch = pltpu.make_async_copy(rows.at[found[0, key % 128]], line, sem)
    fetch.start()
    for index in every:
        fetch_piece(*index).wait()
        put_piece(*index).start()
    fetch.wait()
    branch[0] = line[0, line.shape[1] - 1]
    size = 2 * most + 2 * QUARTERS
    for index in range(size):
        at = index
        if index >= 2 * most:
            final = index - 2 * most
            at = 2 * most + (final + QUARTERS * crossed) % (2 * QUARTERS)
        code = line[0, chip * size + at]
        turned = (code + QUARTERS * swap) % (2 * QUARTERS)
        plan[4 + index] = jnp.where(code < 2 * QUARTERS, turned, code)
    for index in every:
        put_piece(*index).wait()


def piece_copies(source, source_slot, held, target_slot, buffer, in_sem, out_sem):
    pieces, halves = in_sem.shape
    size = buffer.shape[1] // pieces

    def fetch(piece, half):
        at = pl.ds(piece * size, size)
        return pltpu.make_async_copy(
            source.at[source_slot, half, at], buffer.at[half, at], in_sem.at[piece, half]
        )

    def put(piece, half):
        at = pl.ds(piece * size, size)
        return pltpu.make_async_copy(
            buffer.at[half, at], held.at[target_slot, half, at], out_sem.at[piece, half]
        )

    return fetch, put, list(itertools.product(range(pieces), range(halves)))


def make_plan(lengths, moving, destination, caches, counts):
    most = counts[-1]
    place, rows, slots = routes(most)
    lines = -(-place.size // 128)
    places = np.zeros((lines * 128,), np.int32)
    places[: place.size] = place
    table = np.zeros((rows.shape[0], 1, 128), np.int32)
    table[:, 0, : rows[0].size] = rows.reshape(rows.shape[0], -1)
    table[:, 0, 127] = np.sum(slots[:, None] > np.array(counts[:-1]), axis=1)
    anywhere = pl.BlockSpec(memory_space=pl.ANY)
    smem = pl.BlockSpec(memory_space=pltpu.SMEM)
    return pl.pallas_call(
        functools.partial(plan_kernel, most=most),
        out_shape=(
            jax.ShapeDtypeStruct((4 + 2 * most + 2 * QUARTERS,), jnp.int32),
            jax.ShapeDtypeStruct((1,), jnp.int32),
            jax.ShapeDtypeStruct(caches.shape, caches.dtype),
        ),
        in_specs=[
            pl.BlockSpec(memory_space=pltpu.VMEM),
            smem,
            smem,
            anywhere,
            anywhere,
            anywhere,
        ],
        out_specs=(smem, smem, anywhere),
        scratch_shapes=[
            pltpu.SMEM((1, 128), jnp.int32),
            pltpu.SMEM((1, 128), jnp.int32),
            pltpu.VMEM(caches.shape[1:], caches.dtype),
            pltpu.SemaphoreType.DMA,
            pltpu.SemaphoreType.DMA((PIECES, caches.shape[1])),
            pltpu.SemaphoreType.DMA((PIECES, caches.shape[1])),
        ],
        name="plan",
    )(
        lengths.T,
        moving,
        destination,
        jnp.asarray(places.reshape(lines, 1, 128)),
        jnp.asarray(table),
        caches,
    )


def route_kernel(
    plan,
    queries_from,
    keys_from,
    values_from,
    caches,
    weight,
    arrived,
    mixed,
    queries,
    keys_new,
    values_new,
    both,
    local,
    give,
    arr,
    stage,
    final,
    hand,
    query_t,
    row_max,
    row_total,
    weighted,
    attended,
    weight_blocks,
    outgoing,
    incoming,
    totals,
    fresh_sem,
    in_sem,
    give_sem,
    gave_sem,
    send_sem,
    recv_sem,
    keep_sem,
    hand_sem,
    got_sem,
    weight_sem,
    out_sem,
    mix_sem,
    *,
    slots,
    most,
):
    own = lax.axis_index("rep")
    part = lax.axis_index("tp")
    parts = weight_blocks.shape[0]
    core = own % 2
    partner = own + 1 - 2 * core
    across = (own + 2 - 4 * ((own // 2) % 2), own + 4 - 8 * (own // 4))
    rows = stage.shape[3]
    span, columns = mixed.shape[1:]
    kv_count = query_t.shape[0]
    group = query_t.shape[2] // span
    run = QUARTERS * rows
    factor = HEAD ** (-0.5) * LOG2E
    leaving = plan[0]

    def fetch(s):
        return pltpu.make_async_copy(
            caches.at[:, :, pl.ds(s * run, run)], both.at[s], in_sem.at[s]
        )

    def load(step):
        at = pl.ds(pl.multiple_of(lax.rem(part + step, parts) * columns, columns), columns)
        return pltpu.make_async_copy(
            weight.at[:, at], weight_blocks.at[step], weight_sem.at[step]
        )

    fresh_copies = [
        pltpu.make_async_copy(source, into, fresh_sem.at[index])
        for index, (source, into) in enumerate(
            ((queries_from, queries), (keys_from, keys_new), (values_from, values_new))
        )
    ]
    for s in range(STREAMS):
        fetch(s).start()
    barrier = pltpu.get_barrier_semaphore()
    peers = [{"rep": partner}] + [{"rep": peer} for peer in across]
    peers += [{"tp": lax.rem(part + step, parts)} for step in range(1, parts)]
    for peer in peers:
        pl.semaphore_signal(
            barrier, inc=1, device_id=peer, device_id_type=pl.DeviceIdType.MESH
        )

    def remote(src, dst, send, recv, peer):
        return pltpu.make_async_remote_copy(
            src_ref=src,
            dst_ref=dst,
            send_sem=send,
            recv_sem=recv,
            device_id=peer,
            device_id_type=pl.DeviceIdType.MESH,
        )

    def share(s):
        return remote(
            give.at[s],
            local.at[s, pl.ds(core * QUARTERS, QUARTERS)],
            give_sem.at[s],
            gave_sem.at[s],
            {"rep": partner},
        )

    def send(link, slot, s):
        return remote(
            stage.at[link, slot, s],
            arr.at[link, slot, s],
            send_sem.at[link, slot, s],
            recv_sem.at[link, slot, s],
            {"rep": across[link]},
        )

    def settle(s, half):
        return pltpu.make_async_copy(
            final.at[s, half],
            arrived.at[0, half, pl.ds(s * run, run)],
            keep_sem.at[s, half],
        )

    def deliver(s):
        return remote(
            hand.at[s],
            final.at[s, core],
            hand_sem.at[s],
            got_sem.at[s],
            {"rep": partner},
        )

    def mix(kind, index, place, target):
        return remote(
            outgoing.at[kind, index],
            incoming.at[kind, place],
            out_sem.at[kind, index],
            mix_sem.at[kind, place],
            {"tp": target},
        )

    def pick(s, upto, codes, write):
        def body(block, carry):
            at = pl.ds(pl.multiple_of(block * BLOCK_ROWS, BLOCK_ROWS), BLOCK_ROWS)
            values = [local[s, 0, at]] * len(codes)
            came = [(home, local[s, home, at]) for home in range(1, 2 * QUARTERS)]
            came += [
                (2 * QUARTERS + 2 * slot + link, arr[link, slot, s, at])
                for slot in range(upto)
                for link in range(2)
            ]
            for here, piece in came:
                values = [
                    lax.select(code == here, piece, value)
                    for code, value in zip(codes, values)
                ]
            for index, value in enumerate(values):
                write(index, block, value)
            return carry

        lax.fori_loop(0, rows // BLOCK_ROWS, body, 0)

    def share_out(s, carry):
        fetch(s).wait()

        def body(block, carry):
            k = block // (rows // BLOCK_ROWS)
            inner = pl.multiple_of(block % (rows // BLOCK_ROWS) * BLOCK_ROWS, BLOCK_ROWS)
            at = pl.ds(pl.multiple_of(block * BLOCK_ROWS, BLOCK_ROWS), BLOCK_ROWS)
            to = pl.ds(inner, BLOCK_ROWS)
            for half, into in ((1 - core, None), (core, core)):
                value = lax.select(
                    leaving == 0, both[s, 0, half, at], both[s, 1, half, at]
                )
                if into is None:
                    give[s, k, to] = value
                else:
                    local[s, core * QUARTERS + k, to] = value
            return carry

        lax.fori_loop(0, run // BLOCK_ROWS, body, 0)

        @pl.when(s == 0)
        def _():
            pl.semaphore_wait(barrier, len(peers))

        share(s).start()

        return carry

    lax.fori_loop(0, STREAMS, share_out, 0)
    for copy in fresh_copies:
        copy.start()
    for step in list(range(1, parts)) + [0]:
        load(step).start()

    def lanes_of(head):
        return slice(head * HEAD, (head + 1) * HEAD)

    def mix_values(values, weights):
        return lax.dot_general(
            values,
            weights.astype(jnp.bfloat16),
            (((0,), (0,)), ((), ())),
            preferred_element_type=jnp.float32,
        )

    def scores_of(head, keys):
        return lax.dot_general(
            keys,
            query_t[head],
            (((1,), (0,)), ((), ())),
            preferred_element_type=jnp.float32,
        )

    def fresh(slot):
        def choose(ref, lanes):
            return lax.select(slot == 0, ref[0, :, lanes], ref[1, :, lanes])

        key_at = lax.broadcasted_iota(jnp.int32, (span, group * span), 0)
        token_at = lax.broadcasted_iota(jnp.int32, (span, group * span), 1) % span
        for head in range(kv_count):
            for member in range(group):
                query_t[head, :, member * span : (member + 1) * span] = choose(
                    queries, lanes_of(head * group + member)
                ).T
            scores = jnp.where(
                key_at <= token_at, scores_of(head, choose(keys_new, lanes_of(head))), masked_score
            )
            new_max = jnp.max(scores, axis=0, keepdims=True)
            weights = jnp.exp2((scores - new_max) * factor)
            row_max[head] = new_max
            row_total[head] = jnp.sum(weights, axis=0, keepdims=True)
            weighted[head] = mix_values(choose(values_new, lanes_of(head)), weights)

    def absorb(start, length, piece):
        every = [scores_of(head, piece(0, head)) for head in range(kv_count)]
        for head, scores in enumerate(every):
            parts_of = [
                scores[at : at + LENGTH_STEP]
                + jnp.where(start + at < length, 0.0, masked_score)
                for at in range(0, scores.shape[0], LENGTH_STEP)
            ]
            old_max = row_max[head]
            new_max = old_max
            for some in parts_of:
                new_max = jnp.maximum(new_max, jnp.max(some, axis=0, keepdims=True))
            rescale = jnp.exp2((old_max - new_max) * factor)
            weights = [jnp.exp2((some - new_max) * factor) for some in parts_of]
            row_max[head] = new_max
            total = row_total[head] * rescale
            for some in weights:
                total = total + jnp.sum(some, axis=0, keepdims=True)
            row_total[head] = total
            rounded = jnp.concatenate([some.astype(jnp.bfloat16) for some in weights], axis=0)
            weighted[head] = weighted[head] * rescale + mix_values(piece(1, head), rounded)

    def finish():
        for head in range(kv_count):
            result = (weighted[head] * (1.0 / row_total[head])).T
            for member in range(group):
                attended[:, lanes_of(head * group + member)] = result[
                    member * span : (member + 1) * span
                ].astype(jnp.bfloat16)

    relayed = parts == 4
    low = part < parts // 2
    edge = (part == 0) | (part == parts - 1)

    def mirror(place):
        return jnp.where(low, place, parts - 1 - place)

    def product(column):
        step = lax.rem(column - part + parts, parts)
        return jnp.dot(
            attended[...], weight_blocks[step], preferred_element_type=jnp.float32
        )

    def spread_direct(kind):
        def body(index, carry):
            column = lax.rem(part + 1 + index, parts)
            if kind == 0:
                load(lax.rem(index + 1, parts)).wait()
            value = product(column)

            @pl.when(index < parts - 1)
            def _():
                outgoing[kind, index] = value.astype(jnp.bfloat16)
                mix(kind, index, part, column).start()

            @pl.when(index == parts - 1)
            def _():
                totals[kind] = value

            return carry

        lax.fori_loop(0, parts, body, 0)

    def collect_direct(kind):
        for step in range(1, parts):
            place = lax.rem(part + step, parts)
            mix(kind, 0, place, place).wait_recv()
            totals[kind] += incoming[kind, place].astype(jnp.float32)

    def spread_relayed(kind):
        def body(index, carry):
            goal = jnp.where(
                edge,
                jnp.where(index < 2, 3 - index, jnp.where(index == 2, 0, 1)),
                jnp.where(index == 0, 2, jnp.where(index == 1, 0, index * 2 - 3)),
            )
            value = product(mirror(goal))
            slot = jnp.where(index < 2, index, 2)

            @pl.when(index == 2)
            def _():
                totals[kind] = value

            @pl.when((index != 2) & ((index < 3) | edge))
            def _():
                outgoing[kind, slot] = value.astype(jnp.bfloat16)

            @pl.when((index == 3) & jnp.logical_not(edge))
            def _():
                mix(kind, 2, parts, part).wait_recv()
                outgoing[kind, slot] = (
                    value + incoming[kind, parts].astype(jnp.float32)
                ).astype(jnp.bfloat16)

            @pl.when(index != 2)
            def _():
                first = edge & (index == 0)
                mix(
                    kind,
                    slot,
                    jnp.where(first, parts, part),
                    mirror(jnp.where(first, 1, goal)),
                ).start()

            return carry

        lax.fori_loop(0, parts, body, 0)

    def collect_relayed(kind):
        def take(place):
            mix(kind, 0, mirror(place), part).wait_recv()
            totals[kind] += incoming[kind, mirror(place)].astype(jnp.float32)

        @pl.when(edge)
        def _():
            take(1)

        @pl.when(jnp.logical_not(edge))
        def _():
            take(0)
            take(3)

        take(2)

    spread_arrived = spread_relayed if relayed else spread_direct
    collect_arrived = collect_relayed if relayed else collect_direct

    staying_blocks = run // BLOCK

    def absorb_staying(s, block):
        inner = pl.multiple_of(block * BLOCK, BLOCK)
        at = pl.ds(inner, BLOCK)

        def piece(half, head):
            return lax.select(
                leaving == 0,
                both[s, 1, half, at, lanes_of(head)],
                both[s, 0, half, at, lanes_of(head)],
            )

        absorb(s * run + inner, plan[1], piece)

    for slot in range(slots):
        codes = [plan[4 + link * most + slot] for link in range(2)]

        def step_of(s, carry):
            if slot == 0:
                share(s).wait_recv()
            else:
                for link in range(2):
                    send(link, slot - 1, s).wait_recv()

            def write(link, block, value):
                at = pl.ds(pl.multiple_of(block * BLOCK_ROWS, BLOCK_ROWS), BLOCK_ROWS)
                stage[link, slot, s, at] = value

            pick(s, slot, codes, write)
            for link in range(2):
                send(link, slot, s).start()
            if 1 <= slot <= staying_blocks:
                absorb_staying(s, slot - 1)
            return carry

        lax.fori_loop(0, STREAMS, step_of, 0)
        if slot == 0:
            for copy in fresh_copies:
                copy.wait()
            fresh(1 - leaving)
        if slot == staying_blocks:
            finish()
            spread_direct(0)
            fresh(leaving)

    def last_step(s, carry):
        @pl.when(s < STREAMS)
        def _():
            for link in range(2):
                send(link, slots - 1, s).wait_recv()
            for k in range(QUARTERS):
                base = 4 + 2 * most + k
                codes = [plan[base + QUARTERS * core], plan[base + QUARTERS * (1 - core)]]

                def write(index, block, value):
                    at = pl.ds(
                        pl.multiple_of(k * rows + block * BLOCK_ROWS, BLOCK_ROWS), BLOCK_ROWS
                    )
                    if index == 0:
                        final[s, core, at] = value
                    else:
                        hand[s, at] = value

                pick(s, slots, codes, write)
            deliver(s).start()

        @pl.when(s > 0)
        def _():
            before = s - 1
            deliver(before).wait_recv()
            for half in range(2):
                settle(before, half).start()

            def body(block, carry):
                inner = pl.multiple_of(block * BLOCK, BLOCK)
                at = pl.ds(inner, BLOCK)
                absorb(
                    before * run + inner,
                    plan[2],
                    lambda half, head: final[before, half, at, lanes_of(head)],
                )
                return carry

            lax.fori_loop(0, staying_blocks, body, 0)

        return carry

    lax.fori_loop(0, STREAMS + 1, last_step, 0)
    finish()
    spread_arrived(1)
    collect_direct(0)
    staying_mixed = totals[0].astype(jnp.bfloat16)
    collect_arrived(1)
    arrived_mixed = totals[1].astype(jnp.bfloat16)
    mixed[0] = lax.select(leaving == 0, arrived_mixed, staying_mixed)
    mixed[1] = lax.select(leaving == 0, staying_mixed, arrived_mixed)
    for kind in range(2):
        for index in range(parts - 1):
            mix(kind, index, part, lax.rem(part + 1, parts)).wait_send()

    def drain(s, carry):
        share(s).wait_send()
        for slot in range(slots):
            for link in range(2):
                send(link, slot, s).wait_send()
        for half in range(2):
            settle(s, half).wait()
        deliver(s).wait_send()
        return carry

    lax.fori_loop(0, STREAMS, drain, 0)


def route(plan, queries, keys_new, values_new, caches, out_weight, slots, most, identity):
    parts = lax.axis_size("tp")
    slot_count, span, features = queries.shape
    depth = out_weight.shape[0]
    columns = out_weight.shape[1] // parts
    halves, cache_rows, width = caches.shape[1:]
    run = cache_rows // STREAMS
    rows = run // QUARTERS
    kv_count = width // HEAD
    grouped = span * features // width
    anywhere = pl.BlockSpec(memory_space=pl.ANY)
    vmem = pl.BlockSpec(memory_space=pltpu.VMEM)
    kind = jnp.bfloat16
    dma = pltpu.SemaphoreType.DMA
    scratch = [
        pltpu.VMEM(queries.shape, kind),
        pltpu.VMEM(keys_new.shape, kind),
        pltpu.VMEM(values_new.shape, kind),
        pltpu.VMEM((STREAMS, slot_count, halves, run, width), kind),
        pltpu.VMEM((STREAMS, 2 * QUARTERS, rows, width), kind),
        pltpu.VMEM((STREAMS, QUARTERS, rows, width), kind),
        pltpu.VMEM((2, slots, STREAMS, rows, width), kind),
        pltpu.VMEM((2, slots, STREAMS, rows, width), kind),
        pltpu.VMEM((STREAMS, halves, run, width), kind),
        pltpu.VMEM((STREAMS, run, width), kind),
        pltpu.VMEM((kv_count, HEAD, grouped), kind),
        pltpu.VMEM((kv_count, 1, grouped), jnp.float32),
        pltpu.VMEM((kv_count, 1, grouped), jnp.float32),
        pltpu.VMEM((kv_count, HEAD, grouped), jnp.float32),
        pltpu.VMEM((span, features), kind),
        pltpu.VMEM((parts, depth, columns), kind),
        pltpu.VMEM((2, parts - 1, span, columns), kind),
        pltpu.VMEM((2, parts + 1, span, columns), kind),
        pltpu.VMEM((2, span, columns), jnp.float32),
        dma((3,)),
        dma((STREAMS,)),
        dma((STREAMS,)),
        dma((STREAMS,)),
        dma((2, slots, STREAMS)),
        dma((2, slots, STREAMS)),
        dma((STREAMS, halves)),
        dma((STREAMS,)),
        dma((STREAMS,)),
        dma((parts,)),
        dma((2, parts - 1)),
        dma((2, parts + 1)),
    ]
    return pl.pallas_call(
        functools.partial(route_kernel, slots=slots, most=most),
        out_shape=(
            jax.ShapeDtypeStruct((1, halves, cache_rows, width), kind),
            jax.ShapeDtypeStruct((slot_count, span, columns), kind),
        ),
        in_specs=[pl.BlockSpec(memory_space=pltpu.SMEM)] + [anywhere] * 5,
        out_specs=(anywhere, vmem),
        scratch_shapes=scratch,
        compiler_params=pltpu.CompilerParams(
            collective_id=identity, has_side_effects=True, vmem_limit_bytes=60 * 1024 * 1024
        ),
        name=f"route{slots}",
    )(plan, queries, keys_new, values_new, caches, out_weight)


def hold_kernel(plan, arrived, mixed, _, out, held, buffer, rows, in_sem, out_sem, mix_sem):
    leaving = plan[0]
    fetch, put, every = piece_copies(arrived, 0, held, leaving, buffer, in_sem, out_sem)
    for index in every:
        fetch(*index).start()
    take = pltpu.make_async_copy(mixed, rows, mix_sem.at[0])
    give = pltpu.make_async_copy(rows, out, mix_sem.at[1])
    take.start()
    for index in every:
        fetch(*index).wait()
        put(*index).start()
    take.wait()
    give.start()
    for index in every:
        put(*index).wait()
    give.wait()


def hold(plan, arrived, mixed, held):
    hbm = pl.BlockSpec(memory_space=pltpu.HBM)
    return pl.pallas_call(
        hold_kernel,
        out_shape=(
            jax.ShapeDtypeStruct(mixed.shape, mixed.dtype),
            jax.ShapeDtypeStruct(held.shape, held.dtype),
        ),
        in_specs=[pl.BlockSpec(memory_space=pltpu.SMEM), hbm, hbm, hbm],
        out_specs=(hbm, hbm),
        scratch_shapes=[
            pltpu.VMEM(held.shape[1:], held.dtype),
            pltpu.VMEM(mixed.shape, mixed.dtype),
            pltpu.SemaphoreType.DMA((PIECES, held.shape[1])),
            pltpu.SemaphoreType.DMA((PIECES, held.shape[1])),
            pltpu.SemaphoreType.DMA((2,)),
        ],
        input_output_aliases={3: 1},
        name="hold",
    )(plan, arrived, mixed, held)


def migrate(queries, keys_new, values_new, caches, lengths, moving, destination, out_weight):
    slot_count = caches.shape[0]
    span = queries.shape[0] // slot_count
    counts = (4, 5, 6, 8)
    plan, branch, held = make_plan(lengths, moving, destination, caches, counts)

    def by_slot(array):
        return array.reshape(slot_count, span, array.shape[1])

    arrived, mixed = lax.switch(
        branch[0],
        [
            functools.partial(route, slots=slots, most=counts[-1], identity=2 + index)
            for index, slots in enumerate(counts)
        ],
        plan,
        by_slot(queries),
        by_slot(keys_new),
        by_slot(values_new),
        caches,
        out_weight,
    )
    mixed, held = hold(plan, arrived, mixed, held)
    return mixed.reshape(slot_count * span, mixed.shape[2]), held


def on_device(queries, keys_new, values_new, caches, lengths, moving, destination, out_weight):
    replicas = lax.axis_size("rep")
    if replicas == 8:
        return migrate(
            queries, keys_new, values_new, caches, lengths, moving, destination, out_weight
        )
    own_index = lax.axis_index("rep")
    slot_count, _, cache_rows, width = caches.shape
    span = queries.shape[0] // slot_count
    kv_count = width // HEAD
    group = queries.shape[1] // width
    leaving_slot = moving[own_index]
    staying_slot = 1 - leaving_slot
    every = jnp.arange(replicas, dtype=jnp.int32)
    source_of = jnp.sum(
        jnp.where(destination[None, :] == every[:, None], every[None, :], 0), axis=1
    )
    anchor = source_of[own_index]
    incoming_length = lengths[anchor, moving[anchor]]
    staying_length = lengths[own_index, staying_slot]
    query_t = (
        queries.reshape(slot_count, span, kv_count, group, HEAD)
        .transpose(0, 2, 4, 3, 1)
        .reshape(slot_count, kv_count, HEAD, group * span)
    )
    keys_by_slot = keys_new.reshape(slot_count, span, width)
    values_by_slot = values_new.reshape(slot_count, span, width)

    def pick(array, slot):
        return lax.dynamic_index_in_dim(array, slot, 0, keepdims=False)

    held, staying_attended = attend_slot(
        jnp.stack([staying_slot, staying_slot, staying_length]),
        caches,
        pick(query_t, staying_slot),
        pick(keys_by_slot, staying_slot),
        pick(values_by_slot, staying_slot),
        None,
        caches.shape,
    )
    leaving = lax.dynamic_index_in_dim(caches, leaving_slot, 0, keepdims=False)
    piece_rows = 2 * cache_rows // replicas
    pieces = leaving.reshape(replicas, piece_rows, width)
    spread = lax.all_to_all(pieces, "rep", split_axis=0, concat_axis=0, tiled=True)
    ordered = jnp.take(spread, source_of, axis=0, mode="clip")
    arrived = lax.all_to_all(ordered, "rep", split_axis=0, concat_axis=0, tiled=True)
    arrived = arrived.reshape(1, 2, cache_rows, width)
    staying_mixed = project(staying_attended, out_weight, 0)
    held, arrived_attended = attend_slot(
        jnp.stack([jnp.zeros_like(leaving_slot), leaving_slot, incoming_length]),
        arrived,
        pick(query_t, leaving_slot),
        pick(keys_by_slot, leaving_slot),
        pick(values_by_slot, leaving_slot),
        held,
        caches.shape,
    )
    arrived_mixed = project(arrived_attended, out_weight, 1)
    mixed = jnp.where(
        leaving_slot == 0,
        jnp.concatenate([arrived_mixed, staying_mixed], axis=0),
        jnp.concatenate([staying_mixed, arrived_mixed], axis=0),
    )
    return (mixed, held)


def solution(mesh):
    in_specs = (
        P("rep", "tp"),
        P("rep", "tp"),
        P("rep", "tp"),
        P("rep", None, None, "tp"),
        P(),
        P(),
        P(),
        P("tp", None),
    )
    out_specs = (P("rep", "tp"), P("rep", None, None, "tp"))
    return jax.shard_map(
        on_device, mesh=mesh, in_specs=in_specs, out_specs=out_specs, check_vma=False
    )
```
